32 devices in a mesh: gz: 4 (over y, x), gy: 4 (over z), gx: 2 (over core).
Axes of the slice: x: 2, y: 2, z: 4, core: 2. Of those that a mesh axis runs over, the one named last changes fastest.
Arguments:
- spins: float32 [2, 64, 192, 256], P(None, 'gz', 'gy', 'gx'), may hold values from -6 to 6
- kicks: float32 [2, 2, 64, 192, 256], P(None, None, 'gz', 'gy', 'gx'), may hold values from -6 to 6
- stiffness: float32 [64, 192, 256], P('gz', 'gy', 'gx'), may hold values from 0.1 to 11, as said below
Outputs:
- final_spins: float32 [2, 64, 192, 256], P(None, 'gz', 'gy', 'gx')
- section_energy: float32 [16], replicated
The draws below stay inside these ranges and needn't reach their ends.
Inputs may be any that keep to these rules, and one draw needn't show every extreme that they name: `stiffness`: positive coupling strengths.
All inputs are finite; a program needn't handle non-finite values.
Results may differ from the reference program's by a relative error of at most 0.0001.
Values sent between devices are 32-bit elements; how exact they have to be, the bound alone decides.
No kernel may reach another device: no remote copies, remote signals or barrier semaphores. Data moves between devices by JAX's collectives and lax.ppermute only.
A program may use at most 128 MiB of HBM per device.

```python
import jax
import jax.numpy as jnp
from jax import lax

SWEEPS = 2
NZ = 64
NY = 192
NX = 256


def draw_stiffness(key, part):
    shape = (NZ, NY, NX)
    zpos = lax.broadcasted_iota(jnp.float32, shape, 0) / NZ
    ypos = lax.broadcasted_iota(jnp.float32, shape, 1) / NY
    xpos = lax.broadcasted_iota(jnp.float32, shape, 2) / NX
    base = jnp.exp(jax.random.uniform(key, shape, jnp.float32, jnp.log(0.1), jnp.log(0.4)))
    ramp = jnp.exp(jnp.log(3.0) * (zpos + ypos + xpos))
    return (base * ramp).astype(jnp.float32)


def block_scale(rng, dims, shards, low, largest):
    gain = 1.0
    for axis_at, blocks in shards:
        heights = jax.random.uniform(jax.random.fold_in(jax.random.fold_in(rng, 6), axis_at), (blocks,), jnp.float32, low / len(shards), largest / len(shards))
        gain = gain * jnp.repeat(jnp.exp(heights), dims[axis_at] // blocks).reshape((-1,) + (1,) * (len(dims) - 1 - axis_at))
    return gain


def scatter_about(stream_key, extent, scale, reach, shards=(), kind=jnp.bfloat16):
    result = scale * jax.random.normal(stream_key, extent, jnp.float32)
    if shards:
        result = result * block_scale(stream_key, extent, shards, -0.22, 0.18)
    return jnp.clip(result, -reach, reach).astype(kind)


def setup_inputs(seed: int = 0) -> dict:
    key_of = jax.random.split(jax.random.key(seed), 4)
    spins = scatter_about(key_of[0], (2, NZ, NY, NX), 1.0, 6.0, ((1, 4), (2, 4), (3, 2)), jnp.float32)
    kicks = scatter_about(key_of[1], (SWEEPS, 2, NZ, NY, NX), 1.0, 6.0, ((2, 4), (3, 4), (4, 2)), jnp.float32)
    stiffness = draw_stiffness(jax.random.fold_in(key_of[3], 71), 0)
    return {"spins": spins, "kicks": kicks, "stiffness": stiffness}


def neighbour_sum(field):
    total = jnp.zeros(field.shape, jnp.float32)
    for axis in range(3):
        for offset in (1, -1):
            total = total + jnp.roll(field, offset, axis)
    return total

def reference(spins, kicks, stiffness):
    shape = stiffness.shape
    zpar = lax.broadcasted_iota(jnp.int32, shape, 0) % 2
    ypar = lax.broadcasted_iota(jnp.int32, shape, 1) % 2
    xpar = lax.broadcasted_iota(jnp.int32, shape, 2) % 2
    colour = 4 * zpar + 2 * ypar + xpar
    first = spins[0]
    second = spins[1]
    sites = jnp.float32(NZ * NY * NX // 8)
    records = []
    for sweep in range(SWEEPS):
        for section in range(8):
            local_a = stiffness * neighbour_sum(first) + kicks[sweep, 0]
            local_b = stiffness * neighbour_sum(second) + kicks[sweep, 1]
            scale = 1.0 / jnp.sqrt(1.0 + local_a * local_a + local_b * local_b)
            new_a = local_a * scale
            new_b = local_b * scale
            member = colour == section
            first = jnp.where(member, new_a, first)
            second = jnp.where(member, new_b, second)
            energy = jnp.sum(jnp.where(member, new_a * local_a + new_b * local_b, jnp.float32(0.0)))
            records.append(-energy / sites)
    return (jnp.stack([first, second]), jnp.stack(records).astype(jnp.float32))
```

```python
import functools

import jax
import jax.numpy as jnp
from jax import lax
from jax.experimental import pallas as pl
from jax.experimental.pallas import tpu as pltpu
from jax.sharding import PartitionSpec as P

SWEEPS = 2
VMEM = pl.BlockSpec(memory_space=pltpu.VMEM)
F32 = jnp.float32

FIRST = (0, 1, 2, 3, 4)
ALL = (0, 1, 2, 3, 4, 5, 6)


def up_planes(depth):
    return [(f, depth - 2) for f in FIRST] + [(f, depth - 1) for f in FIRST]


def down_planes():
    return [(f, 0) for f in ALL] + [(f, 1) for f in FIRST] + [(f, 2) for f in FIRST]


def load_field(s_ref, k_ref, st_ref, field, z, rows=slice(None)):
    if field < 2:
        return s_ref[field, z, rows, :]
    if field == 2:
        return st_ref[z, rows, :]
    return k_ref[(field - 3) // 2, (field - 3) % 2, z, rows, :]


def pack_kernel(s_ref, k_ref, st_ref, zup, zdn, yup, ydn, cuu, cud, cdu, cdd):
    depth, height, lanes = st_ref.shape
    for out, planes, far in ((zup, up_planes(depth), depth - 2), (zdn, down_planes(), 2)):
        beyond = depth - 3 if far == depth - 2 else 3
        for n, (field, z) in enumerate(planes):
            value = load_field(s_ref, k_ref, st_ref, field, z)
            if z == far and field in (3, 4):
                value = value + st_ref[z] * s_ref[field - 3, beyond]
            out[n] = value
    sub = lax.broadcasted_iota(jnp.int32, (8, lanes), 0)
    quad = sub % 4
    order = (quad % 2) * 2 + quad // 2
    lower = sub < 4

    def merge(a, b, base):
        a = jnp.take_along_axis(a, order + base, axis=0)
        b = jnp.take_along_axis(b, order + base, axis=0)
        return jnp.where(lower, a, b)

    first, last = slice(0, 8), slice(height - 8, height)
    for src, hi, lo, count in ((zup, cud, cuu, 10), (zdn, cdd, cdu, 17)):
        for n in range(0, count, 2):
            m = min(n + 1, count - 1)
            hi[n // 2] = merge(src[n, first, :], src[m, first, :], 0)
            lo[n // 2] = merge(src[n, last, :], src[m, last, :], 4)
    get = functools.partial(load_field, s_ref, k_ref, st_ref)
    half = depth // 2
    for field in ALL:
        for p in range(half):
            ydn[field * half + p] = merge(get(field, 2 * p, first), get(field, 2 * p + 1, first), 0)
            if field in FIRST:
                yup[field * half + p] = merge(get(field, 2 * p, last), get(field, 2 * p + 1, last), 4)


def pack(spins, kicks, stiffness):
    depth, height, lanes = stiffness.shape
    shapes = [
        (10, height, lanes),
        (17, height, lanes),
        (5 * depth // 2, 8, lanes),
        (7 * depth // 2, 8, lanes),
        (5, 8, lanes),
        (5, 8, lanes),
        (9, 8, lanes),
        (9, 8, lanes),
    ]
    return pl.pallas_call(
        pack_kernel,
        out_shape=[jax.ShapeDtypeStruct(s, F32) for s in shapes],
        in_specs=[VMEM] * 3,
        out_specs=[VMEM] * 8,
        compiler_params=pltpu.CompilerParams(vmem_limit_bytes=16 << 20),
        cost_estimate=pl.CostEstimate(flops=1_000_000, bytes_accessed=4_000_000, transcendentals=0),
        name="pack",
    )(spins, kicks, stiffness)


def sweep_kernel(*refs):
    own, other = refs[:11], refs[11:22]
    out, energies = refs[22:24]
    S, ST, K, E = refs[24:]
    depth, height, lanes = own[2].shape
    half, rows = height // 2, S.shape[4]
    planes = depth + 7
    lane = lax.broadcasted_iota(jnp.int32, (8, lanes), 1)
    sub = lax.broadcasted_iota(jnp.int32, (8, lanes), 0)
    mid = lanes // 2
    left8 = lane < mid
    lower8 = sub < 4
    own8 = jnp.where(left8, 2 * lane, 2 * (lane - mid) + 1)
    other8 = jnp.where(left8, 2 * lane + 1, 2 * (lane - mid))

    def tall(v, n=rows):
        return jnp.concatenate([v] * (n // 8), axis=0)

    left, own_index, other_index = tall(left8.astype(jnp.int32)) > 0, tall(own8), tall(other8)

    def put(field, zi, y, x, value):
        if field < 2:
            S[field, y, x, zi] = value
        elif field == 2:
            ST[y, x, zi] = value
        else:
            K[field - 3, y, x, zi] = value

    def edge(hi, lo, part, y):
        shift = -(4 * part + 2 * y)
        value = hi if shift == 0 else pltpu.roll(hi, shift % 8, 0)
        if lo is None:
            return value
        shift = (6 - 4 * part) if y == 0 else (4 - 4 * part)
        return jnp.where(lower8, value, lo if shift == 0 else pltpu.roll(lo, shift, 0))

    def place(field, zi, body, hi, lo, part):
        for y in (0, 1):
            a = jnp.concatenate([body(0, y), edge(hi(0), lo and lo(0), part, y)], axis=0)
            b = jnp.concatenate([body(1, y), edge(hi(1), lo and lo(1), part, y)], axis=0)
            a = jnp.take_along_axis(a, own_index, axis=1)
            b = jnp.take_along_axis(b, other_index, axis=1)
            put(field, zi, y, 0, jnp.where(left, a, b))
            put(field, zi, y, 1, pltpu.roll(jnp.where(left, b, a), mid, 1))

    sides = (own, other)
    for c in range(2):
        for y in range(2):
            for x in range(2):
                S[c, y, x, 0] = jnp.zeros((rows, lanes), F32)
                S[c, y, x, planes - 1] = jnp.zeros((rows, lanes), F32)

    def pair(p, carry):
        for field in ALL:
            for part in (0, 1):
                z = 2 * p + part
                place(
                    field,
                    z + 3,
                    lambda i, y: load_field(*sides[i][:3], field, z, pl.ds(y, half, stride=2)),
                    lambda i: sides[i][6][field * (depth // 2) + p],
                    (lambda i: sides[i][5][field * (depth // 2) + p]) if field in FIRST else None,
                    part,
                )
        return carry

    lax.fori_loop(0, depth // 2, pair, 0)
    for which, listed, base in ((3, up_planes(depth), -depth), (4, down_planes(), depth)):
        for n, (field, z) in enumerate(listed):
            lo, hi = (7, 8) if which == 3 else (9, 10)
            place(
                field,
                z + base + 3,
                lambda i, y: sides[i][which][n, pl.ds(y, half, stride=2), :],
                lambda i: sides[i][hi][n // 2],
                lambda i: sides[i][lo][n // 2],
                n % 2,
            )

    for t in range(8 * SWEEPS):
        sweep, colour = divmod(t, 8)
        zp, yp, xp = colour // 4, (colour // 2) % 2, colour % 2
        reach = 2 * (SWEEPS - 1 - sweep)
        start = zp - reach
        stop = depth - zp + reach
        count = (stop - start) // 2 + 1

        def step(i, acc):
            z = start + 2 * i
            zi = z + 3
            stiff = ST[yp, xp, zi]
            local = []
            for c in (0, 1):
                along = S[c, yp, 1 - xp, zi]
                total = along + pltpu.roll(along, 1 if xp == 0 else lanes - 1, 1)
                across = S[c, 1 - yp, xp, zi]
                total = total + (across + pltpu.roll(across, 1 if yp == 0 else rows - 1, 0))
                total = total + (S[c, yp, xp, zi - 1] + S[c, yp, xp, zi + 1])
                local.append(stiff * total + K[2 * sweep + c, yp, xp, zi])
            square = local[0] * local[0] + local[1] * local[1]
            scale = lax.rsqrt(1.0 + square)
            for c in (0, 1):
                S[c, yp, xp, zi] = local[c] * scale
            energy = (square * scale)[:half]
            energy = sum(energy[8 * j : 8 * j + 8] for j in range(half // 8))
            return acc + jnp.where((z >= 0) & (z < depth), energy, 0.0)

        acc = lax.fori_loop(0, count, step, jnp.zeros((8, lanes), F32))
        E[pl.ds(t, 1), :] = jnp.sum(jnp.where(left8, acc, 0.0), axis=0, keepdims=True)

    total = jnp.sum(E[...], axis=1, keepdims=True)
    shape = E.shape
    diagonal = lax.broadcasted_iota(jnp.int32, shape, 0) == lax.broadcasted_iota(jnp.int32, shape, 1)
    line = jnp.sum(jnp.where(diagonal, total, 0.0), axis=0, keepdims=True)
    energies[...] = jnp.broadcast_to(line, energies.shape)

    inverse8 = lane // 2 + mid * (lane % 2)
    left_half, inverse = tall(left8.astype(jnp.int32), half) > 0, tall(inverse8, half)

    def write(z, carry):
        for c in (0, 1):
            for y in (0, 1):
                even, odd = S[c, y, 0, z + 3, :half], S[c, y, 1, z + 3, :half]
                value = jnp.where(left_half, even, pltpu.roll(odd, mid, 1))
                out[c, z, pl.ds(y, half, stride=2), :] = jnp.take_along_axis(value, inverse, axis=1)
        return carry

    lax.fori_loop(0, depth, write, 0)


def sweeps(own, other, devices):
    stiffness = own[2]
    depth, height, lanes = stiffness.shape
    rows = -(-(height // 2 + 4) // 8) * 8
    planes = depth + 7
    return pl.pallas_call(
        sweep_kernel,
        out_shape=[
            jax.ShapeDtypeStruct(own[0].shape, F32),
            jax.ShapeDtypeStruct((devices, lanes), F32),
        ],
        in_specs=[VMEM] * 22,
        out_specs=[VMEM] * 2,
        scratch_shapes=[
            pltpu.VMEM((2, 2, 2, planes, rows, lanes), F32),
            pltpu.VMEM((2, 2, planes, rows, lanes), F32),
            pltpu.VMEM((2 * SWEEPS, 2, 2, planes, rows, lanes), F32),
            pltpu.VMEM((8 * SWEEPS, lanes), F32),
        ],
        compiler_params=pltpu.CompilerParams(vmem_limit_bytes=32 << 20),
        cost_estimate=pl.CostEstimate(flops=50_000_000, bytes_accessed=10_000_000, transcendentals=0),
        name="sweeps",
    )(*own, *other)


def body(spins, kicks, stiffness):
    nz, ny, nx = (lax.axis_size(a) for a in ("gz", "gy", "gx"))
    devices = nz * ny * nx
    sites = jnp.float32(stiffness.size * devices // 8)

    def shift(value, dz, dy):
        pairs = [
            (z * ny + y, (z + dz) % nz * ny + (y + dy) % ny) for z in range(nz) for y in range(ny)
        ]
        return lax.ppermute(value, ("gz", "gy"), pairs)

    lanes = stiffness.shape[-1]

    def beside(value):
        right = lax.ppermute(value, "gx", [((i + 1) % nx, i) for i in range(nx)])
        if nx == 2:
            return right
        left = lax.ppermute(value, "gx", [(i, (i + 1) % nx) for i in range(nx)])
        lane = lax.broadcasted_iota(jnp.int32, value.shape, value.ndim - 1)
        return jnp.where(lane < lanes // 2, right, left)

    raw = (spins, kicks, stiffness)
    zup, zdn, yup, ydn, cuu, cud, cdu, cdd = pack(*raw)
    halo = (
        shift(zup, 1, 0),
        shift(zdn, -1, 0),
        shift(yup, 0, 1),
        shift(ydn, 0, -1),
        shift(cuu, 1, 1),
        shift(cud, 1, -1),
        shift(cdu, -1, 1),
        shift(cdd, -1, -1),
    )
    own = raw + halo
    other = tuple(beside(v) for v in own)
    final, energies = sweeps(own, other, devices)
    parts = lax.all_to_all(energies, ("gz", "gy", "gx"), 0, 0, tiled=True)
    total = jnp.sum(parts, axis=0)[: 8 * SWEEPS]
    return (final, -total / sites)


def solution(mesh):
    placed = (P(None, "gz", "gy", "gx"), P(None, None, "gz", "gy", "gx"), P("gz", "gy", "gx"))
    return jax.shard_map(
        body,
        mesh=mesh,
        in_specs=placed,
        out_specs=(P(None, "gz", "gy", "gx"), P()),
        check_vma=False,
    )
```

```python
import functools

import jax
import jax.numpy as jnp
from jax import lax
from jax.experimental import pallas as pl
from jax.experimental.pallas import tpu as pltpu
from jax.sharding import PartitionSpec as P


SWEEPS = 2
FACE_GRANT = 55_000_000
EDGE_GRANT = 8_000_000
VMEM = pl.BlockSpec(memory_space=pltpu.VMEM)
F32 = jnp.float32

FIRST = (0, 1, 2, 3, 4)
ALL = (0, 1, 2, 3, 4, 5, 6)


def up_planes(depth):
    return [(f, z) for f in FIRST for z in (depth - 2, depth - 1)]


def down_planes():
    return [(f, z) for f in FIRST for z in (0, 1, 2)] + [(5, 0), (6, 0)]


CORNERS = {"cuu": 0, "cud": 5, "cdu": 10, "cdd": 19, "end": 28}


def load_field(s_ref, k_ref, st_ref, field, z, rows=slice(None)):
    return field_ref(s_ref, k_ref, st_ref, field)[z, rows, :]


def field_ref(s_ref, k_ref, st_ref, field):
    if field < 2:
        return s_ref.at[field]
    if field == 2:
        return st_ref
    return k_ref.at[(field - 3) // 2, (field - 3) % 2]


def copy_all(moves, sems):
    copies = [pltpu.make_async_copy(a, b, sems.at[i]) for i, (a, b) in enumerate(moves)]
    for c in copies:
        c.start()
    for c in copies:
        c.wait()


def face_kernel(s_ref, k_ref, st_ref, zup, zdn, far, sems):
    depth, _, _ = st_ref.shape
    get = functools.partial(field_ref, s_ref, k_ref, st_ref)
    moves = [(s_ref.at[:, depth - 3], far.at[0]), (s_ref.at[:, 3], far.at[1])]
    for f in FIRST:
        moves.append((get(f).at[pl.ds(0, 3)], zdn.at[pl.ds(3 * f, 3)]))
        moves.append((get(f).at[pl.ds(depth - 2, 2)], zup.at[pl.ds(2 * f, 2)]))
    moves += [(get(5).at[pl.ds(0, 1)], zdn.at[pl.ds(15, 1)]), (get(6).at[pl.ds(0, 1)], zdn.at[pl.ds(16, 1)])]
    copy_all(moves, sems)
    for c in (0, 1):
        n = 2 * (3 + c)
        zup[n] = zup[n] + zup[4] * far[0, c]
        n = 3 * (3 + c) + 2
        zdn[n] = zdn[n] + zdn[8] * far[1, c]


def edge_kernel(s_ref, k_ref, st_ref, zup, zdn, up, down, corners, s_low, s_high, k_low, k_high, t_low, t_high, sems):
    depth, height, lanes = st_ref.shape
    first, last = pl.ds(0, 8), pl.ds(height - 8, 8)
    copy_all(
        [
            (s_ref.at[:, :, first], s_low),
            (s_ref.at[:, :, last], s_high),
            (k_ref.at[:, :, :, first], k_low),
            (k_ref.at[0, :, :, last], k_high),
            (st_ref.at[:, first], t_low),
            (st_ref.at[:, last], t_high),
        ],
        sems,
    )
    sub = lax.broadcasted_iota(jnp.int32, (8, lanes), 0)
    quad = sub % 4
    order = (quad % 2) * 2 + quad // 2
    lower = sub < 4

    def merge(a, b, base):
        a = jnp.take_along_axis(a, order + base, axis=0)
        b = jnp.take_along_axis(b, order + base, axis=0)
        return jnp.where(lower, a, b)

    at = CORNERS
    for src, hi, lo, count in ((zup, at["cud"], at["cuu"], 10), (zdn, at["cdd"], at["cdu"], 17)):
        for n in range(0, count, 2):
            m = min(n + 1, count - 1)
            corners[hi + n // 2] = merge(src[n, first, :], src[m, first, :], 0)
            corners[lo + n // 2] = merge(src[n, last, :], src[m, last, :], 4)

    def row(field, z, is_low):
        s, k, t = (s_low, k_low, t_low) if is_low else (s_high, k_high, t_high)
        if field < 2:
            return s[field, z]
        if field == 2:
            return t[z]
        c = (field - 3) % 2
        if not is_low:
            return k[c, z] + jnp.where(sub == 6, t[z] * pltpu.roll(s[c, z], 1, 0), 0.0)
        if field > 4:
            return k[1, c, z]
        return k[0, c, z] + jnp.where(sub == 2, t[z] * pltpu.roll(s[c, z], 7, 0), 0.0)

    for field in FIRST:
        for p in range(depth // 2):
            tile = merge(row(field, 2 * p, True), row(field, 2 * p + 1, True), 0)
            if field < 2:
                a, b = (pltpu.roll(row(5 + field, 2 * p + i, True), 3 + 4 * i, 0) for i in (0, 1))
                tile = jnp.where(quad == 3, jnp.where(lower, a, b), tile)
            down[field * (depth // 2) + p] = tile
        for q in range(depth // 4):
            tile = row(field, 4 * q + 3, False)
            for i in range(3):
                tile = jnp.where(sub // 2 == i, pltpu.roll(row(field, 4 * q + i, False), (2 * i + 2) % 8, 0), tile)
            up[field * (depth // 4) + q] = tile


def pack_faces(spins, kicks, stiffness):
    _, height, lanes = stiffness.shape
    return pl.pallas_call(
        face_kernel,
        out_shape=[jax.ShapeDtypeStruct((n, height, lanes), F32) for n in (10, 17)],
        in_specs=[pl.BlockSpec(memory_space=pltpu.HBM)] * 3,
        out_specs=[VMEM] * 2,
        scratch_shapes=[pltpu.VMEM((2, 2, height, lanes), F32), pltpu.SemaphoreType.DMA((14,))],
        compiler_params=pltpu.CompilerParams(vmem_limit_bytes=FACE_GRANT),
        cost_estimate=pl.CostEstimate(flops=1_000_000, bytes_accessed=1_000_000, transcendentals=0),
        name="faces",
    )(spins, kicks, stiffness)


def pack_edges(spins, kicks, stiffness, zup, zdn):
    depth, _, lanes = stiffness.shape
    return pl.pallas_call(
        edge_kernel,
        out_shape=[jax.ShapeDtypeStruct((n, 8, lanes), F32) for n in (5 * depth // 4, 5 * depth // 2, CORNERS["end"])],
        in_specs=[pl.BlockSpec(memory_space=pltpu.HBM)] * 3 + [VMEM] * 2,
        out_specs=[VMEM] * 3,
        scratch_shapes=[
            pltpu.VMEM((2, depth, 8, lanes), F32),
            pltpu.VMEM((2, depth, 8, lanes), F32),
            pltpu.VMEM((SWEEPS, 2, depth, 8, lanes), F32),
            pltpu.VMEM((2, depth, 8, lanes), F32),
            pltpu.VMEM((depth, 8, lanes), F32),
            pltpu.VMEM((depth, 8, lanes), F32),
            pltpu.SemaphoreType.DMA((6,)),
        ],
        compiler_params=pltpu.CompilerParams(vmem_limit_bytes=EDGE_GRANT),
        cost_estimate=pl.CostEstimate(flops=1_000_000, bytes_accessed=2_000_000, transcendentals=0),
        name="edges",
    )(spins, kicks, stiffness, zup, zdn)


def small_call(kernel, shapes, *args):
    return pl.pallas_call(
        kernel,
        out_shape=[jax.ShapeDtypeStruct(s, F32) for s in shapes],
        in_specs=[VMEM] * len(args),
        out_specs=[VMEM] * len(shapes),
        compiler_params=pltpu.CompilerParams(vmem_limit_bytes=4 << 20),
        cost_estimate=pl.CostEstimate(flops=100_000, bytes_accessed=1_000_000, transcendentals=0),
    )(*args)


def per_core(moves):
    core = lax.axis_index("gx") % 2
    for c in (0, 1):

        @pl.when(core == c)
        def _():
            for target, at, source, start, count in moves[c]:
                target[at : at + count] = source[start : start + count]


def share_out(lanes, mine, pair):
    def spread(mine, pair, first, second):
        moves = ([], [])
        for core, parts in ((0, (("cdd", 9, first), ("cdu", 9, second))), (1, (("cuu", 5, first), ("cud", 5, second)))):
            for name, count, target in parts:
                moves[core].append((target, 0, mine, CORNERS[name], count))
                moves[core].append((target, 9, pair, CORNERS[name], count))
        per_core(moves)

    return small_call(spread, [(18, 8, lanes)] * 2, mine, pair)


def join(lo, hi):
    def join_edges(lo, hi, out):
        out[: lo.shape[0]] = lo[...]
        out[lo.shape[0] :] = hi[...]

    return small_call(join_edges, [(lo.shape[0] + hi.shape[0], *lo.shape[1:])], lo, hi)[0]


def stack_corners(lanes, first, second):
    def stack(first, second, out):
        out[:18] = first[...]
        out[18:] = second[...]

    return small_call(stack, [(36, 8, lanes)], first, second)[0]


def sort_corners(lanes, got, pair):
    def sort_c(got, pair, own, other):
        moves = ([], [])
        for place, count, start, core in ((0, 5, 0, 1), (5, 5, 18, 1), (10, 9, 18, 0), (19, 9, 0, 0)):
            for c in (0, 1):
                source, flip = (got, 0) if c == core else (pair, 9)
                moves[c].append((own, place, source, start + flip, count))
                moves[c].append((other, place, source, start + 9 - flip, count))
        per_core(moves)

    return small_call(sort_c, [(28, 8, lanes)] * 2, got, pair)


class Rows:
    def __init__(self, S, ST, K, depth, height):
        self.S, self.ST, self.K = S, ST, K
        self.depth, self.height = depth, height
        self.half = height // 2
        self.rows, self.lanes = S.shape[4:]
        lane = lax.broadcasted_iota(jnp.int32, (8, self.lanes), 1)
        self.lane = lane
        self.sub = lax.broadcasted_iota(jnp.int32, (8, self.lanes), 0)
        self.lower8 = self.sub < 4
        self.even = lax.broadcasted_iota(jnp.int32, (self.rows, self.lanes), 1) % 2 == 0
        end = self.lanes - 1
        before = jnp.where(lane == 0, 0, jnp.where(lane == 1, end, lane - 1))
        after = jnp.where(lane == 0, 0, jnp.where(lane == end, 1, lane + 1))
        self.before = jnp.concatenate([before] * (self.rows // 8), axis=0)
        self.after = jnp.concatenate([after] * (self.rows // 8), axis=0)

    def put(self, field, zi, y, x, value):
        if field < 2:
            self.S[field, y, x, zi] = value
        elif field == 2:
            self.ST[y, x, zi] = value
        else:
            self.K[field - 3, y, x, zi] = value

    def edge(self, hi, lo, part, y):
        shift = -(4 * part + 2 * y)
        value = hi if shift == 0 else pltpu.roll(hi, shift % 8, 0)
        shift = (6 - 4 * part) if y == 0 else (4 - 4 * part)
        return jnp.where(self.lower8, value, lo if shift == 0 else pltpu.roll(lo, shift, 0))

    def rows_beyond(self, hi, lo, j, y, second_kick):
        base = 4 * (j % 2)
        if second_kick:
            return pltpu.roll(hi, (-base - 3) % 8, 0) if y == 0 else jnp.zeros(hi.shape, F32)
        above, below = (-base - 2 * y) % 8, 7 - 2 * j - y
        above = pltpu.roll(hi, above, 0) if above else hi
        below = pltpu.roll(lo, below % 8, 0) if below % 8 else lo
        return jnp.where(self.sub < 2 - y, above, jnp.where(self.sub == 7, below, 0.0))

    def place(self, field, zi, body, beyond):
        for y in (0, 1):
            a = jnp.concatenate([body(0, y), beyond(0, y)], axis=0)
            b = jnp.concatenate([body(1, y), beyond(1, y)], axis=0)
            b = pltpu.roll(b, 1, 1)
            self.put(field, zi, y, 0, jnp.where(self.even, a, b))
            self.put(field, zi, y, 1, jnp.where(self.even, b, a))

    def section(self, t, planes):
        S, ST, K = self.S, self.ST, self.K
        sweep, colour = divmod(t, 8)
        yp, xp = (colour // 2) % 2, colour % 2
        acc = jnp.zeros((8, self.lanes), F32)
        for z in planes:
            zi = z + 3
            stiff = ST[yp, xp, zi]
            local = []
            for c in (0, 1):
                along = S[c, yp, 1 - xp, zi]
                if xp == 0:
                    total = jnp.take_along_axis(along, self.before, axis=1) + pltpu.roll(along, self.lanes - 1, 1)
                else:
                    total = jnp.take_along_axis(along, self.after, axis=1) + pltpu.roll(along, 1, 1)
                across = S[c, 1 - yp, xp, zi]
                total = total + (across + pltpu.roll(across, 1 if yp == 0 else self.rows - 1, 0))
                total = total + (S[c, yp, xp, zi - 1] + S[c, yp, xp, zi + 1])
                local.append(stiff * total + K[2 * sweep + c, yp, xp, zi])
            square = local[0] * local[0] + local[1] * local[1]
            scale = lax.rsqrt(1.0 + square)
            for c in (0, 1):
                S[c, yp, xp, zi] = local[c] * scale
            if 0 <= z < self.depth:
                energy = (square * scale)[: self.half]
                acc = acc + sum(energy[8 * j : 8 * j + 8] for j in range(self.half // 8))
        return acc


def inner_planes(depth, t):
    phase = t // 4
    return range(2 + phase, depth - 1 - phase, 2)


def outer_planes(depth, t):
    phase = t // 4
    reach = 2 * (SWEEPS - 1 - t // 8)
    parity = phase % 2
    return [z for z in range(parity - reach, depth - parity + reach + 1, 2) if z not in inner_planes(depth, t)]


def middle_kernel(*refs):
    own, other = refs[:4], refs[4:8]
    S, ST, K, E = refs[8:]
    depth, height, _ = own[2].shape
    rows = Rows(S, ST, K, depth, height)
    sides = (own, other)
    high = 5 * depth // 4

    def four(q, carry):
        for field in ALL:
            source = field if field in FIRST else field - 5
            for j in range(4):
                rows.place(
                    field,
                    4 * q + j + 3,
                    lambda i, y: load_field(*sides[i][:3], field, 4 * q + j, pl.ds(y, height // 2, stride=2)),
                    lambda i, y: rows.rows_beyond(
                        sides[i][3][high + source * (depth // 2) + 2 * q + j // 2],
                        sides[i][3][source * (depth // 4) + q],
                        j,
                        y,
                        field not in FIRST,
                    ),
                )
        return carry

    lax.fori_loop(0, depth // 4, four, 0)
    for t in range(8 * SWEEPS):
        E[t] = rows.section(t, inner_planes(depth, t))


def middle(own, other):
    depth, height, lanes = own[2].shape
    rows = -(-(height // 2 + 4) // 8) * 8
    planes = depth + 7
    return pl.pallas_call(
        middle_kernel,
        out_shape=[
            jax.ShapeDtypeStruct((2, 2, 2, planes, rows, lanes), F32),
            jax.ShapeDtypeStruct((2, 2, planes, rows, lanes), F32),
            jax.ShapeDtypeStruct((2 * SWEEPS, 2, 2, planes, rows, lanes), F32),
            jax.ShapeDtypeStruct((8 * SWEEPS, 8, lanes), F32),
        ],
        in_specs=[VMEM] * 8,
        out_specs=[VMEM] * 4,
        compiler_params=pltpu.CompilerParams(vmem_limit_bytes=8 << 20),
        cost_estimate=pl.CostEstimate(flops=30_000_000, bytes_accessed=10_000_000, transcendentals=0),
        name="middle",
    )(*own, *other)


def last_kernel(*refs):
    E = refs[3]
    own, other = refs[4:7], refs[7:10]
    S, ST, K, out, energies, lines = refs[10:]
    depth, height, lanes = out.shape[1:]
    rows = Rows(S, ST, K, depth, height)
    sides = (own, other)
    for c in range(2):
        for y in range(2):
            for x in range(2):
                S[c, y, x, 0] = jnp.zeros((rows.rows, lanes), F32)
                S[c, y, x, depth + 6] = jnp.zeros((rows.rows, lanes), F32)
    for which, listed, base, lo in ((0, up_planes(depth), -depth, 0), (1, down_planes(), depth, 10)):
        for n, (field, z) in enumerate(listed):
            hi = lo + (5, 9)[which]
            rows.place(
                field,
                z + base + 3,
                lambda i, y: sides[i][which][n, pl.ds(y, height // 2, stride=2), :],
                lambda i, y: rows.edge(sides[i][2][hi + n // 2], sides[i][2][lo + n // 2], n % 2, y),
            )
    for t in range(8 * SWEEPS):
        acc = E[t] + rows.section(t, outer_planes(depth, t))
        mine = rows.lane % 2 == t % 2
        lines[pl.ds(t, 1), :] = jnp.sum(jnp.where(mine, acc, 0.0), axis=0, keepdims=True)

    total = jnp.sum(lines[...], axis=1, keepdims=True)
    diagonal = lax.broadcasted_iota(jnp.int32, lines.shape, 0) == lax.broadcasted_iota(jnp.int32, lines.shape, 1)
    line = jnp.sum(jnp.where(diagonal, total, 0.0), axis=0, keepdims=True)
    energies[...] = jnp.broadcast_to(line, energies.shape)
    half = height // 2

    def write(z, carry):
        for c in (0, 1):
            for y in (0, 1):
                value = jnp.where(rows.even[:half], S[c, y, 0, z + 3, :half], S[c, y, 1, z + 3, :half])
                out[c, z, pl.ds(y, half, stride=2), :] = value
        return carry

    lax.fori_loop(0, depth, write, 0)


def last(state, own, other, shape, devices):
    lanes = shape[-1]
    results = pl.pallas_call(
        last_kernel,
        out_shape=[jax.ShapeDtypeStruct(v.shape, F32) for v in state[:3]]
        + [jax.ShapeDtypeStruct(shape, F32), jax.ShapeDtypeStruct((devices, lanes), F32)],
        in_specs=[VMEM] * 10,
        out_specs=[VMEM] * 5,
        input_output_aliases={0: 0, 1: 1, 2: 2},
        scratch_shapes=[pltpu.VMEM((8 * SWEEPS, lanes), F32)],
        compiler_params=pltpu.CompilerParams(vmem_limit_bytes=8 << 20),
        cost_estimate=pl.CostEstimate(flops=30_000_000, bytes_accessed=10_000_000, transcendentals=0),
        name="last",
    )(*state, *own, *other)
    return results[3:]


def step(spins, kicks, stiffness):
    nz, ny, nx = (lax.axis_size(a) for a in ("gz", "gy", "gx"))
    devices = nz * ny * nx
    sites = jnp.float32(stiffness.size * devices // 8)

    def shift(value, even_core, odd_core):
        pairs = []
        for z in range(nz):
            for y in range(ny):
                for x in range(nx):
                    dz, dy = odd_core if x % 2 else even_core
                    pairs.append(((z * ny + y) * nx + x, ((z + dz) % nz * ny + (y + dy) % ny) * nx + x))
        return lax.ppermute(value, ("gz", "gy", "gx"), pairs)

    def swap(value):
        return lax.ppermute(value, "gx", [(i, i ^ 1) for i in range(nx)])

    lanes = stiffness.shape[-1]

    def beside(value):
        right = lax.ppermute(value, "gx", [((i + 1) % nx, i) for i in range(nx)])
        if nx == 2:
            return right
        left = lax.ppermute(value, "gx", [(i, (i + 1) % nx) for i in range(nx)])
        lane = lax.broadcasted_iota(jnp.int32, value.shape, value.ndim - 1)
        return jnp.where(lane < lanes // 2, right, left)

    raw = (spins, kicks, stiffness)
    zup, zdn = pack_faces(*raw)
    yup, ydn, mine = pack_edges(*raw, zup, zdn)
    first, second = share_out(lanes, mine, swap(mine))
    up, down, left, right = (1, 0), (-1, 0), (0, -1), (0, 1)
    zlo, zhi = shift(zup, up, up), shift(zdn, down, down)
    edges = join(shift(yup, right, right), shift(ydn, left, left))
    corners = stack_corners(lanes, shift(first, (-1, -1), (1, 1)), shift(second, (-1, 1), (1, -1)))
    beyond = beside(edges)
    other = tuple(beside(v) for v in raw)
    state = middle(raw + (edges,), other + (beyond,))
    corners, beyond = sort_corners(lanes, corners, swap(corners))
    if nx > 2:
        beyond = beside(corners)
    other = (beside(zlo), beside(zhi), beyond)
    final, energies = last(state, (zlo, zhi, corners), other, spins.shape, devices)
    parts = lax.all_to_all(energies, ("gz", "gy", "gx"), 0, 0, tiled=True)
    total = jnp.sum(parts, axis=0)[: 8 * SWEEPS]
    return (final, -total / sites)


def solution(mesh):
    placed = (P(None, "gz", "gy", "gx"), P(None, None, "gz", "gy", "gx"), P("gz", "gy", "gx"))
    return jax.shard_map(
        step,
        mesh=mesh,
        in_specs=placed,
        out_specs=(P(None, "gz", "gy", "gx"), P()),
        check_vma=False,
    )
```

```python
import functools

import jax
import jax.numpy as jnp
from jax import lax
from jax.experimental import pallas as pl
from jax.experimental.pallas import tpu as pltpu
from jax.sharding import PartitionSpec as P


SWEEPS = 2
FACE_GRANT = 55_000_000
EDGE_GRANT = 8_000_000
VMEM = pl.BlockSpec(memory_space=pltpu.VMEM)
F32 = jnp.float32

FIRST = (0, 1, 2, 3, 4)
ALL = (0, 1, 2, 3, 4, 5, 6)


def up_planes(depth):
    return [(f, z) for f in FIRST for z in (depth - 2, depth - 1)]


def down_planes():
    return [(f, z) for f in FIRST for z in (0, 1, 2)] + [(5, 0), (6, 0)]


CORNERS = {"cuu": 0, "cud": 5, "cdu": 10, "cdd": 19, "end": 28}


def load_field(s_ref, k_ref, st_ref, field, z, rows=slice(None)):
    return field_ref(s_ref, k_ref, st_ref, field)[z, rows, :]


def field_ref(s_ref, k_ref, st_ref, field):
    if field < 2:
        return s_ref.at[field]
    if field == 2:
        return st_ref
    return k_ref.at[(field - 3) // 2, (field - 3) % 2]


def copy_all(moves, sems):
    copies = [pltpu.make_async_copy(a, b, sems.at[i]) for i, (a, b) in enumerate(moves)]
    for c in copies:
        c.start()
    for c in copies:
        c.wait()


def face_kernel(s_ref, k_ref, st_ref, zup, zdn, far, sems):
    depth, _, _ = st_ref.shape
    get = functools.partial(field_ref, s_ref, k_ref, st_ref)
    moves = [(s_ref.at[:, depth - 3], far.at[0]), (s_ref.at[:, 3], far.at[1])]
    for f in FIRST:
        moves.append((get(f).at[pl.ds(0, 3)], zdn.at[pl.ds(3 * f, 3)]))
        moves.append((get(f).at[pl.ds(depth - 2, 2)], zup.at[pl.ds(2 * f, 2)]))
    moves += [(get(5).at[pl.ds(0, 1)], zdn.at[pl.ds(15, 1)]), (get(6).at[pl.ds(0, 1)], zdn.at[pl.ds(16, 1)])]
    copy_all(moves, sems)
    for c in (0, 1):
        n = 2 * (3 + c)
        zup[n] = zup[n] + zup[4] * far[0, c]
        n = 3 * (3 + c) + 2
        zdn[n] = zdn[n] + zdn[8] * far[1, c]


def edge_kernel(s_ref, k_ref, st_ref, zup, zdn, up, down, corners, s_low, s_high, k_low, k_high, t_low, t_high, sems):
    depth, height, lanes = st_ref.shape
    first, last = pl.ds(0, 8), pl.ds(height - 8, 8)
    copy_all(
        [
            (s_ref.at[:, :, first], s_low),
            (s_ref.at[:, :, last], s_high),
            (k_ref.at[:, :, :, first], k_low),
            (k_ref.at[0, :, :, last], k_high),
            (st_ref.at[:, first], t_low),
            (st_ref.at[:, last], t_high),
        ],
        sems,
    )
    sub = lax.broadcasted_iota(jnp.int32, (8, lanes), 0)
    quad = sub % 4
    order = (quad % 2) * 2 + quad // 2
    lower = sub < 4

    def merge(a, b, base):
        a = jnp.take_along_axis(a, order + base, axis=0)
        b = jnp.take_along_axis(b, order + base, axis=0)
        return jnp.where(lower, a, b)

    at = CORNERS
    for src, hi, lo, count in ((zup, at["cud"], at["cuu"], 10), (zdn, at["cdd"], at["cdu"], 17)):
        for n in range(0, count, 2):
            m = min(n + 1, count - 1)
            corners[hi + n // 2] = merge(src[n, first, :], src[m, first, :], 0)
            corners[lo + n // 2] = merge(src[n, last, :], src[m, last, :], 4)

    def row(field, z, is_low):
        s, k, t = (s_low, k_low, t_low) if is_low else (s_high, k_high, t_high)
        if field < 2:
            return s[field, z]
        if field == 2:
            return t[z]
        c = (field - 3) % 2
        if not is_low:
            return k[c, z] + jnp.where(sub == 6, t[z] * pltpu.roll(s[c, z], 1, 0), 0.0)
        if field > 4:
            return k[1, c, z]
        return k[0, c, z] + jnp.where(sub == 2, t[z] * pltpu.roll(s[c, z], 7, 0), 0.0)

    for field in FIRST:
        for p in range(depth // 2):
            tile = merge(row(field, 2 * p, True), row(field, 2 * p + 1, True), 0)
            if field < 2:
                a, b = (pltpu.roll(row(5 + field, 2 * p + i, True), 3 + 4 * i, 0) for i in (0, 1))
                tile = jnp.where(quad == 3, jnp.where(lower, a, b), tile)
            down[field * (depth // 2) + p] = tile
        for q in range(depth // 4):
            tile = row(field, 4 * q + 3, False)
            for i in range(3):
                tile = jnp.where(sub // 2 == i, pltpu.roll(row(field, 4 * q + i, False), (2 * i + 2) % 8, 0), tile)
            up[field * (depth // 4) + q] = tile


def pack_faces(spins, kicks, stiffness):
    _, height, lanes = stiffness.shape
    return pl.pallas_call(
        face_kernel,
        out_shape=[jax.ShapeDtypeStruct((n, height, lanes), F32) for n in (10, 17)],
        in_specs=[pl.BlockSpec(memory_space=pltpu.HBM)] * 3,
        out_specs=[VMEM] * 2,
        scratch_shapes=[pltpu.VMEM((2, 2, height, lanes), F32), pltpu.SemaphoreType.DMA((14,))],
        compiler_params=pltpu.CompilerParams(vmem_limit_bytes=FACE_GRANT),
        cost_estimate=pl.CostEstimate(flops=1_000_000, bytes_accessed=1_000_000, transcendentals=0),
        name="faces",
    )(spins, kicks, stiffness)


def pack_edges(spins, kicks, stiffness, zup, zdn):
    depth, _, lanes = stiffness.shape
    return pl.pallas_call(
        edge_kernel,
        out_shape=[jax.ShapeDtypeStruct((n, 8, lanes), F32) for n in (5 * depth // 4, 5 * depth // 2, CORNERS["end"])],
        in_specs=[pl.BlockSpec(memory_space=pltpu.HBM)] * 3 + [VMEM] * 2,
        out_specs=[VMEM] * 3,
        scratch_shapes=[
            pltpu.VMEM((2, depth, 8, lanes), F32),
            pltpu.VMEM((2, depth, 8, lanes), F32),
            pltpu.VMEM((SWEEPS, 2, depth, 8, lanes), F32),
            pltpu.VMEM((2, depth, 8, lanes), F32),
            pltpu.VMEM((depth, 8, lanes), F32),
            pltpu.VMEM((depth, 8, lanes), F32),
            pltpu.SemaphoreType.DMA((6,)),
        ],
        compiler_params=pltpu.CompilerParams(vmem_limit_bytes=EDGE_GRANT),
        cost_estimate=pl.CostEstimate(flops=1_000_000, bytes_accessed=2_000_000, transcendentals=0),
        name="edges",
    )(spins, kicks, stiffness, zup, zdn)


def small_call(kernel, shapes, *args):
    return pl.pallas_call(
        kernel,
        out_shape=[jax.ShapeDtypeStruct(s, F32) for s in shapes],
        in_specs=[VMEM] * len(args),
        out_specs=[VMEM] * len(shapes),
        compiler_params=pltpu.CompilerParams(vmem_limit_bytes=4 << 20),
        cost_estimate=pl.CostEstimate(flops=100_000, bytes_accessed=1_000_000, transcendentals=0),
    )(*args)


def per_core(moves):
    core = lax.axis_index("gx") % 2
    for c in (0, 1):

        @pl.when(core == c)
        def _():
            for target, at, source, start, count in moves[c]:
                target[at : at + count] = source[start : start + count]


def share_out(lanes, mine, pair):
    def spread(mine, pair, first, second):
        moves = ([], [])
        for core, parts in ((0, (("cdd", 9, first), ("cdu", 9, second))), (1, (("cuu", 5, first), ("cud", 5, second)))):
            for name, count, target in parts:
                moves[core].append((target, 0, mine, CORNERS[name], count))
                moves[core].append((target, 9, pair, CORNERS[name], count))
        per_core(moves)

    return small_call(spread, [(18, 8, lanes)] * 2, mine, pair)


def join(lo, hi):
    def join_edges(lo, hi, out):
        out[: lo.shape[0]] = lo[...]
        out[lo.shape[0] :] = hi[...]

    return small_call(join_edges, [(lo.shape[0] + hi.shape[0], *lo.shape[1:])], lo, hi)[0]


def stack_corners(lanes, first, second):
    def stack(first, second, out):
        out[:18] = first[...]
        out[18:] = second[...]

    return small_call(stack, [(36, 8, lanes)], first, second)[0]


def sort_corners(lanes, got, pair):
    def sort_c(got, pair, own, other):
        moves = ([], [])
        for place, count, start, core in ((0, 5, 0, 1), (5, 5, 18, 1), (10, 9, 18, 0), (19, 9, 0, 0)):
            for c in (0, 1):
                source, flip = (got, 0) if c == core else (pair, 9)
                moves[c].append((own, place, source, start + flip, count))
                moves[c].append((other, place, source, start + 9 - flip, count))
        per_core(moves)

    return small_call(sort_c, [(28, 8, lanes)] * 2, got, pair)


class Rows:
    def __init__(self, S, ST, K, depth, height):
        self.S, self.ST, self.K = S, ST, K
        self.depth, self.height = depth, height
        self.half = height // 2
        self.rows, self.lanes = S.shape[4:]
        lane = lax.broadcasted_iota(jnp.int32, (8, self.lanes), 1)
        self.lane = lane
        self.sub = lax.broadcasted_iota(jnp.int32, (8, self.lanes), 0)
        self.lower8 = self.sub < 4
        self.even = lax.broadcasted_iota(jnp.int32, (self.rows, self.lanes), 1) % 2 == 0
        end = self.lanes - 1
        before = jnp.where(lane == 0, 0, jnp.where(lane == 1, end, lane - 1))
        after = jnp.where(lane == 0, 0, jnp.where(lane == end, 1, lane + 1))
        self.before = jnp.concatenate([before] * (self.rows // 8), axis=0)
        self.after = jnp.concatenate([after] * (self.rows // 8), axis=0)

    def put(self, field, zi, y, start, a, b):
        b = pltpu.roll(b, 1, 1)
        even = self.even[: a.shape[0]]
        for x in (0, 1):
            value = jnp.where(even, a, b) if x == 0 else jnp.where(even, b, a)
            at = (y, x, zi, pl.ds(start, a.shape[0]))
            if field < 2:
                self.S[(field, *at)] = value
            elif field == 2:
                self.ST[at] = value
            else:
                self.K[(field - 3, *at)] = value

    def edge(self, hi, lo, part, y):
        shift = -(4 * part + 2 * y)
        value = hi if shift == 0 else pltpu.roll(hi, shift % 8, 0)
        shift = (6 - 4 * part) if y == 0 else (4 - 4 * part)
        return jnp.where(self.lower8, value, lo if shift == 0 else pltpu.roll(lo, shift, 0))

    def rows_beyond(self, hi, lo, j, y, second_kick):
        base = 4 * (j % 2)
        if second_kick:
            return pltpu.roll(hi, (-base - 3) % 8, 0) if y == 0 else jnp.zeros(hi.shape, F32)
        above, below = (-base - 2 * y) % 8, 7 - 2 * j - y
        above = pltpu.roll(hi, above, 0) if above else hi
        below = pltpu.roll(lo, below % 8, 0) if below % 8 else lo
        return jnp.where(self.sub < 2 - y, above, jnp.where(self.sub == 7, below, 0.0))

    def section(self, t, planes):
        S, ST, K = self.S, self.ST, self.K
        sweep, colour = divmod(t, 8)
        yp, xp = (colour // 2) % 2, colour % 2
        acc = jnp.zeros((8, self.lanes), F32)
        for z in planes:
            zi = z + 3
            stiff = ST[yp, xp, zi]
            local = []
            for c in (0, 1):
                along = S[c, yp, 1 - xp, zi]
                if xp == 0:
                    total = jnp.take_along_axis(along, self.before, axis=1) + pltpu.roll(along, self.lanes - 1, 1)
                else:
                    total = jnp.take_along_axis(along, self.after, axis=1) + pltpu.roll(along, 1, 1)
                across = S[c, 1 - yp, xp, zi]
                total = total + (across + pltpu.roll(across, 1 if yp == 0 else self.rows - 1, 0))
                total = total + (S[c, yp, xp, zi - 1] + S[c, yp, xp, zi + 1])
                local.append(stiff * total + K[2 * sweep + c, yp, xp, zi])
            square = local[0] * local[0] + local[1] * local[1]
            scale = lax.rsqrt(1.0 + square)
            for c in (0, 1):
                S[c, yp, xp, zi] = local[c] * scale
            if 0 <= z < self.depth:
                energy = (square * scale)[: self.half]
                acc = acc + sum(energy[8 * j : 8 * j + 8] for j in range(self.half // 8))
        return acc


def inner_planes(depth, t):
    phase = t // 4
    return range(2 + phase, depth - 1 - phase, 2)


def outer_planes(depth, t):
    phase = t // 4
    reach = 2 * (SWEEPS - 1 - t // 8)
    parity = phase % 2
    return [z for z in range(parity - reach, depth - parity + reach + 1, 2) if z not in inner_planes(depth, t)]


def build_kernel(*refs):
    own, other = refs[:3], refs[3:6]
    S, ST, K = refs[6:]
    depth, height, _ = own[2].shape
    rows = Rows(S, ST, K, depth, height)

    def two(p, carry):
        for field in ALL:
            for z in (2 * p, 2 * p + 1):
                for y in (0, 1):
                    a, b = (load_field(*side, field, z, pl.ds(y, height // 2, stride=2)) for side in (own, other))
                    rows.put(field, z + 3, y, 0, a, b)
        return carry

    lax.fori_loop(0, depth // 2, two, 0)


def build(own, other):
    depth, height, lanes = own[2].shape
    rows = -(-(height // 2 + 4) // 8) * 8
    planes = depth + 7
    return pl.pallas_call(
        build_kernel,
        out_shape=[
            jax.ShapeDtypeStruct((2, 2, 2, planes, rows, lanes), F32),
            jax.ShapeDtypeStruct((2, 2, planes, rows, lanes), F32),
            jax.ShapeDtypeStruct((2 * SWEEPS, 2, 2, planes, rows, lanes), F32),
        ],
        in_specs=[VMEM] * 6,
        out_specs=[VMEM] * 3,
        compiler_params=pltpu.CompilerParams(vmem_limit_bytes=8 << 20),
        cost_estimate=pl.CostEstimate(flops=30_000_000, bytes_accessed=10_000_000, transcendentals=0),
        name="build",
    )(*own, *other)


def middle_kernel(*refs):
    sides = refs[3:5]
    height = 2 * refs[5][0]
    S, ST, K, E = refs[6:]
    depth = S.shape[3] - 7
    rows = Rows(S, ST, K, depth, height)
    high = 5 * depth // 4

    def four(q, carry):
        for field in ALL:
            source = field if field in FIRST else field - 5
            for j in range(4):
                for y in (0, 1):
                    a, b = (
                        rows.rows_beyond(
                            side[high + source * (depth // 2) + 2 * q + j // 2],
                            side[source * (depth // 4) + q],
                            j,
                            y,
                            field not in FIRST,
                        )
                        for side in sides
                    )
                    rows.put(field, 4 * q + j + 3, y, height // 2, a, b)
        return carry

    lax.fori_loop(0, depth // 4, four, 0)
    for t in range(8 * SWEEPS):
        E[t] = rows.section(t, inner_planes(depth, t))


def middle(state, own, other, height):
    lanes = own.shape[-1]

    def kernel(*refs):
        middle_kernel(*refs[:5], (height // 2,), *refs[5:])

    return pl.pallas_call(
        kernel,
        out_shape=[jax.ShapeDtypeStruct(v.shape, F32) for v in state] + [jax.ShapeDtypeStruct((8 * SWEEPS, 8, lanes), F32)],
        in_specs=[VMEM] * 5,
        out_specs=[VMEM] * 4,
        input_output_aliases={0: 0, 1: 1, 2: 2},
        compiler_params=pltpu.CompilerParams(vmem_limit_bytes=8 << 20),
        cost_estimate=pl.CostEstimate(flops=30_000_000, bytes_accessed=10_000_000, transcendentals=0),
        name="middle",
    )(*state, own, other)


def last_kernel(*refs):
    E = refs[3]
    own, other = refs[4:7], refs[7:10]
    S, ST, K, out, energies, lines, final, sems = refs[10:]
    depth, height, lanes = out.shape[1:]
    rows = Rows(S, ST, K, depth, height)
    sides = (own, other)
    for c in range(2):
        for y in range(2):
            for x in range(2):
                S[c, y, x, 0] = jnp.zeros((rows.rows, lanes), F32)
                S[c, y, x, depth + 6] = jnp.zeros((rows.rows, lanes), F32)
    for which, listed, base, lo in ((0, up_planes(depth), -depth, 0), (1, down_planes(), depth, 10)):
        for n, (field, z) in enumerate(listed):
            hi = lo + (5, 9)[which]
            for y in (0, 1):
                a, b = (
                    jnp.concatenate(
                        [
                            side[which][n, pl.ds(y, height // 2, stride=2), :],
                            rows.edge(side[2][hi + n // 2], side[2][lo + n // 2], n % 2, y),
                        ],
                        axis=0,
                    )
                    for side in sides
                )
                rows.put(field, z + base + 3, y, 0, a, b)
    half = height // 2
    sent = []

    def send(start, stop):
        for z in range(start, stop):
            for c in (0, 1):
                for y in (0, 1):
                    value = jnp.where(rows.even[:half], S[c, y, 0, z + 3, :half], S[c, y, 1, z + 3, :half])
                    final[c, z, pl.ds(y, half, stride=2), :] = value
        part = pl.ds(start, stop - start)
        copy = pltpu.make_async_copy(final.at[:, part], out.at[:, part], sems.at[len(sent)])
        copy.start()
        sent.append(copy)

    low, high = 2 * SWEEPS, depth - 2 * SWEEPS + 1
    send(low, high)
    for t in range(8 * SWEEPS):
        acc = E[t] + rows.section(t, outer_planes(depth, t))
        mine = rows.lane % 2 == t % 2
        lines[pl.ds(t, 1), :] = jnp.sum(jnp.where(mine, acc, 0.0), axis=0, keepdims=True)

    send(0, low)
    send(high, depth)
    total = jnp.sum(lines[...], axis=1, keepdims=True)
    diagonal = lax.broadcasted_iota(jnp.int32, lines.shape, 0) == lax.broadcasted_iota(jnp.int32, lines.shape, 1)
    line = jnp.sum(jnp.where(diagonal, total, 0.0), axis=0, keepdims=True)
    energies[...] = jnp.broadcast_to(line, energies.shape)
    for copy in sent:
        copy.wait()


def last(state, own, other, shape, devices):
    lanes = shape[-1]
    results = pl.pallas_call(
        last_kernel,
        out_shape=[jax.ShapeDtypeStruct(v.shape, F32) for v in state[:3]]
        + [jax.ShapeDtypeStruct(shape, F32), jax.ShapeDtypeStruct((devices, lanes), F32)],
        in_specs=[VMEM] * 10,
        out_specs=[VMEM] * 3 + [pl.BlockSpec(memory_space=pltpu.HBM), VMEM],
        input_output_aliases={0: 0, 1: 1, 2: 2},
        scratch_shapes=[
            pltpu.VMEM((8 * SWEEPS, lanes), F32),
            pltpu.VMEM(shape, F32),
            pltpu.SemaphoreType.DMA((3,)),
        ],
        compiler_params=pltpu.CompilerParams(vmem_limit_bytes=8 << 20),
        cost_estimate=pl.CostEstimate(flops=30_000_000, bytes_accessed=10_000_000, transcendentals=0),
        name="last",
    )(*state, *own, *other)
    return results[3:]


def step(spins, kicks, stiffness):
    nz, ny, nx = (lax.axis_size(a) for a in ("gz", "gy", "gx"))
    devices = nz * ny * nx
    sites = jnp.float32(stiffness.size * devices // 8)

    def shift(value, even_core, odd_core):
        pairs = []
        for z in range(nz):
            for y in range(ny):
                for x in range(nx):
                    dz, dy = odd_core if x % 2 else even_core
                    pairs.append(((z * ny + y) * nx + x, ((z + dz) % nz * ny + (y + dy) % ny) * nx + x))
        return lax.ppermute(value, ("gz", "gy", "gx"), pairs)

    def swap(value):
        return lax.ppermute(value, "gx", [(i, i ^ 1) for i in range(nx)])

    lanes = stiffness.shape[-1]

    def beside(value):
        right = lax.ppermute(value, "gx", [((i + 1) % nx, i) for i in range(nx)])
        if nx == 2:
            return right
        left = lax.ppermute(value, "gx", [(i, (i + 1) % nx) for i in range(nx)])
        lane = lax.broadcasted_iota(jnp.int32, value.shape, value.ndim - 1)
        return jnp.where(lane < lanes // 2, right, left)

    raw = (spins, kicks, stiffness)
    zup, zdn = pack_faces(*raw)
    yup, ydn, mine = pack_edges(*raw, zup, zdn)
    first, second = share_out(lanes, mine, swap(mine))
    up, down, left, right = (1, 0), (-1, 0), (0, -1), (0, 1)
    zlo, zhi = shift(zup, up, up), shift(zdn, down, down)
    edges = join(shift(yup, right, right), shift(ydn, left, left))
    corners = stack_corners(lanes, shift(first, (-1, -1), (1, 1)), shift(second, (-1, 1), (1, -1)))
    beyond = beside(edges)
    other = tuple(beside(v) for v in raw)
    state = build(raw, other)
    state = middle(state, edges, beyond, stiffness.shape[1])
    corners, beyond = sort_corners(lanes, corners, swap(corners))
    if nx > 2:
        beyond = beside(corners)
    other = (beside(zlo), beside(zhi), beyond)
    final, energies = last(state, (zlo, zhi, corners), other, spins.shape, devices)
    parts = lax.all_to_all(energies, ("gz", "gy", "gx"), 0, 0, tiled=True)
    total = jnp.sum(parts, axis=0)[: 8 * SWEEPS]
    return (final, -total / sites)


def solution(mesh):
    placed = (P(None, "gz", "gy", "gx"), P(None, None, "gz", "gy", "gx"), P("gz", "gy", "gx"))
    return jax.shard_map(
        step,
        mesh=mesh,
        in_specs=placed,
        out_specs=(P(None, "gz", "gy", "gx"), P()),
        check_vma=False,
    )
```

```python
import functools

import jax
import jax.numpy as jnp
from jax import lax
from jax.experimental import pallas as pl
from jax.experimental.pallas import tpu as pltpu
from jax.sharding import PartitionSpec as P


SWEEPS = 2
FACE_GRANT = 56_000_000
EDGE_GRANT = 8_000_000
VMEM = pl.BlockSpec(memory_space=pltpu.VMEM)
F32 = jnp.float32

FIRST = (0, 1, 2, 3, 4)
ALL = (0, 1, 2, 3, 4, 5, 6)


def up_planes(depth):
    return [(f, z) for f in FIRST for z in (depth - 2, depth - 1)]


def down_planes():
    return [(f, z) for f in FIRST for z in (0, 1, 2)] + [(5, 0), (6, 0)]


CORNERS = {"cuu": (0, 1), "cud": (1, 2), "cdu": (3, 3), "cdd": (6, 5)}
CORNER_TILES = 11


def corner_rows(name):
    if name == "cuu":
        spins, first, second = {1: (-1, -2), 0: (-1,)}, {}, ()
    elif name == "cud":
        spins, first, second = {1: (0, 1, 2), 0: (0, 1)}, {1: (0,), 0: (0,)}, ()
    elif name == "cdu":
        spins, first, second = {0: (-1, -2, -3), 1: (-1, -2), 2: (-1,)}, {0: (-1, -2)}, ()
    else:
        spins, first, second = {0: (0, 1, 2, 3), 1: (0, 1, 2), 2: (0, 1)}, {0: (0, 1, 2), 1: (0,), 2: (0,)}, (0,)
    planes = 2 if name[1] == "u" else 3
    listed = [(planes * f + z, r) for f in FIRST for z, rows in (spins if f < 2 else first).items() for r in rows]
    return listed + [(n, r) for n in (15, 16) for r in second]


def load_field(s_ref, k_ref, st_ref, field, z, rows=slice(None)):
    return field_ref(s_ref, k_ref, st_ref, field)[z, rows, :]


def field_ref(s_ref, k_ref, st_ref, field):
    if field < 2:
        return s_ref.at[field]
    if field == 2:
        return st_ref
    return k_ref.at[(field - 3) // 2, (field - 3) % 2]


def copy_all(moves, sems):
    copies = [pltpu.make_async_copy(a, b, sems.at[i]) for i, (a, b) in enumerate(moves)]
    for c in copies:
        c.start()
    for c in copies:
        c.wait()


def face_kernel(s_ref, k_ref, st_ref, zup, zdn, far, sems):
    depth, _, _ = st_ref.shape
    get = functools.partial(field_ref, s_ref, k_ref, st_ref)
    moves = [(s_ref.at[:, depth - 3], far.at[0]), (s_ref.at[:, 3], far.at[1])]
    for f in FIRST:
        moves.append((get(f).at[pl.ds(0, 3)], zdn.at[pl.ds(3 * f, 3)]))
        moves.append((get(f).at[pl.ds(depth - 2, 2)], zup.at[pl.ds(2 * f, 2)]))
    moves += [(get(5).at[pl.ds(0, 1)], zdn.at[pl.ds(15, 1)]), (get(6).at[pl.ds(0, 1)], zdn.at[pl.ds(16, 1)])]
    copy_all(moves, sems)
    for c in (0, 1):
        n = 2 * (3 + c)
        zup[n] = zup[n] + zup[4] * far[0, c]
        n = 3 * (3 + c) + 2
        zdn[n] = zdn[n] + zdn[8] * far[1, c]


def edge_kernel(s_ref, k_ref, st_ref, zup, zdn, up, down, corners, s_low, s_high, k_low, k_high, t_low, t_high, sems):
    depth, height, lanes = st_ref.shape
    first, last = pl.ds(0, 8), pl.ds(height - 8, 8)
    copy_all(
        [
            (s_ref.at[:, :, first], s_low),
            (s_ref.at[:, :, last], s_high),
            (k_ref.at[:, :, :, first], k_low),
            (k_ref.at[0, :, :, last], k_high),
            (st_ref.at[:, first], t_low),
            (st_ref.at[:, last], t_high),
        ],
        sems,
    )
    sub = lax.broadcasted_iota(jnp.int32, (8, lanes), 0)
    quad = sub % 4
    order = (quad % 2) * 2 + quad // 2
    lower = sub < 4

    def merge(a, b, base):
        a = jnp.take_along_axis(a, order + base, axis=0)
        b = jnp.take_along_axis(b, order + base, axis=0)
        return jnp.where(lower, a, b)

    for name, (start, count) in CORNERS.items():
        src = zup if name[1] == "u" else zdn
        tiles = [jnp.zeros((8, lanes), F32)] * count
        for i, (n, r) in enumerate(corner_rows(name)):
            value, place = (src[n, first, :], r) if r >= 0 else (src[n, last, :], 8 + r)
            shift = (i - place) % 8
            value = pltpu.roll(value, shift, 0) if shift else value
            tiles[i // 8] = jnp.where(sub == i % 8, value, tiles[i // 8])
        for i in range(count):
            corners[start + i] = tiles[i]

    def row(field, z, is_low):
        s, k, t = (s_low, k_low, t_low) if is_low else (s_high, k_high, t_high)
        if field < 2:
            return s[field, z]
        if field == 2:
            return t[z]
        c = (field - 3) % 2
        if not is_low:
            return k[c, z] + jnp.where(sub == 6, t[z] * pltpu.roll(s[c, z], 1, 0), 0.0)
        if field > 4:
            return k[1, c, z]
        return k[0, c, z] + jnp.where(sub == 2, t[z] * pltpu.roll(s[c, z], 7, 0), 0.0)

    for field in FIRST:
        for p in range(depth // 2):
            tile = merge(row(field, 2 * p, True), row(field, 2 * p + 1, True), 0)
            if field < 2:
                a, b = (pltpu.roll(row(5 + field, 2 * p + i, True), 3 + 4 * i, 0) for i in (0, 1))
                tile = jnp.where(quad == 3, jnp.where(lower, a, b), tile)
            down[field * (depth // 2) + p] = tile
        for q in range(depth // 4):
            tile = row(field, 4 * q + 3, False)
            for i in range(3):
                tile = jnp.where(sub // 2 == i, pltpu.roll(row(field, 4 * q + i, False), (2 * i + 2) % 8, 0), tile)
            up[field * (depth // 4) + q] = tile


def pack_faces(spins, kicks, stiffness):
    _, height, lanes = stiffness.shape
    return pl.pallas_call(
        face_kernel,
        out_shape=[jax.ShapeDtypeStruct((n, height, lanes), F32) for n in (10, 17)],
        in_specs=[pl.BlockSpec(memory_space=pltpu.HBM)] * 3,
        out_specs=[VMEM] * 2,
        scratch_shapes=[pltpu.VMEM((2, 2, height, lanes), F32), pltpu.SemaphoreType.DMA((14,))],
        compiler_params=pltpu.CompilerParams(vmem_limit_bytes=FACE_GRANT),
        cost_estimate=pl.CostEstimate(flops=1_000_000, bytes_accessed=1_000_000, transcendentals=0),
        name="faces",
    )(spins, kicks, stiffness)


def pack_edges(spins, kicks, stiffness, zup, zdn):
    depth, _, lanes = stiffness.shape
    return pl.pallas_call(
        edge_kernel,
        out_shape=[jax.ShapeDtypeStruct((n, 8, lanes), F32) for n in (5 * depth // 4, 5 * depth // 2, CORNER_TILES)],
        in_specs=[pl.BlockSpec(memory_space=pltpu.HBM)] * 3 + [VMEM] * 2,
        out_specs=[VMEM] * 3,
        scratch_shapes=[
            pltpu.VMEM((2, depth, 8, lanes), F32),
            pltpu.VMEM((2, depth, 8, lanes), F32),
            pltpu.VMEM((SWEEPS, 2, depth, 8, lanes), F32),
            pltpu.VMEM((2, depth, 8, lanes), F32),
            pltpu.VMEM((depth, 8, lanes), F32),
            pltpu.VMEM((depth, 8, lanes), F32),
            pltpu.SemaphoreType.DMA((6,)),
        ],
        compiler_params=pltpu.CompilerParams(vmem_limit_bytes=EDGE_GRANT),
        cost_estimate=pl.CostEstimate(flops=1_000_000, bytes_accessed=2_000_000, transcendentals=0),
        name="edges",
    )(spins, kicks, stiffness, zup, zdn)


def small_call(kernel, shapes, *args):
    return pl.pallas_call(
        kernel,
        out_shape=[jax.ShapeDtypeStruct(s, F32) for s in shapes],
        in_specs=[VMEM] * len(args),
        out_specs=[VMEM] * len(shapes),
        compiler_params=pltpu.CompilerParams(vmem_limit_bytes=4 << 20),
        cost_estimate=pl.CostEstimate(flops=100_000, bytes_accessed=1_000_000, transcendentals=0),
    )(*args)


def per_core(moves):
    core = lax.axis_index("gx") % 2
    for c in (0, 1):

        @pl.when(core == c)
        def _():
            for target, at, source, start, count in moves[c]:
                target[at : at + count] = source[start : start + count]


def share_out(lanes, mine, pair):
    def spread(mine, pair, first, second):
        moves = ([], [])
        for core, parts in ((0, (("cdd", first), ("cud", second))), (1, (("cdu", first), ("cuu", second)))):
            for name, target in parts:
                start, count = CORNERS[name]
                moves[core].append((target, 0, mine, start, count))
                moves[core].append((target, target.shape[0] // 2, pair, start, count))
        per_core(moves)

    return small_call(spread, [(10, 8, lanes), (4, 8, lanes)], mine, pair)


def join(lo, hi):
    def join_edges(lo, hi, out):
        out[: lo.shape[0]] = lo[...]
        out[lo.shape[0] :] = hi[...]

    return small_call(join_edges, [(lo.shape[0] + hi.shape[0], *lo.shape[1:])], lo, hi)[0]


def stack_corners(lanes, first, second):
    def stack(first, second, out):
        out[:10] = first[...]
        out[10:] = second[...]

    return small_call(stack, [(14, 8, lanes)], first, second)[0]


def sort_corners(lanes, got, pair):
    def sort_c(got, pair, own, other):
        moves = ([], [])
        for name, start, half, core in (("cdd", 0, 5, 0), ("cdu", 0, 5, 1), ("cud", 10, 2, 0), ("cuu", 10, 2, 1)):
            place, count = CORNERS[name]
            for c in (0, 1):
                source, flip = (got, 0) if c == core else (pair, half)
                moves[c].append((own, place, source, start + flip, count))
                moves[c].append((other, place, source, start + half - flip, count))
        per_core(moves)

    return small_call(sort_c, [(CORNER_TILES, 8, lanes)] * 2, got, pair)


class Rows:
    def __init__(self, S, ST, K, depth, height):
        self.S, self.ST, self.K = S, ST, K
        self.depth, self.height = depth, height
        self.half = height // 2
        self.rows, self.lanes = S.shape[4:]
        lane = lax.broadcasted_iota(jnp.int32, (8, self.lanes), 1)
        self.lane = lane
        self.sub = lax.broadcasted_iota(jnp.int32, (8, self.lanes), 0)
        self.even = lax.broadcasted_iota(jnp.int32, (self.rows, self.lanes), 1) % 2 == 0
        end = self.lanes - 1
        before = jnp.where(lane == 0, 0, jnp.where(lane == 1, end, lane - 1))
        after = jnp.where(lane == 0, 0, jnp.where(lane == end, 1, lane + 1))
        self.before = jnp.concatenate([before] * (self.rows // 8), axis=0)
        self.after = jnp.concatenate([after] * (self.rows // 8), axis=0)

    def put(self, field, zi, y, start, a, b):
        b = pltpu.roll(b, 1, 1)
        even = self.even[: a.shape[0]]
        for x in (0, 1):
            value = jnp.where(even, a, b) if x == 0 else jnp.where(even, b, a)
            at = (y, x, zi, pl.ds(start, a.shape[0]))
            if field < 2:
                self.S[(field, *at)] = value
            elif field == 2:
                self.ST[at] = value
            else:
                self.K[(field - 3, *at)] = value

    def corner(self, tiles, names, n, y):
        value = jnp.zeros((8, self.lanes), F32)
        for name in names:
            for i, (m, r) in enumerate(corner_rows(name)):
                if m == n and r % 2 == y:
                    place = r // 2 if r >= 0 else {-1: 7, -2: 7, -3: 6}[r]
                    tile = tiles[CORNERS[name][0] + i // 8]
                    shift = (place - i) % 8
                    tile = pltpu.roll(tile, shift, 0) if shift else tile
                    value = jnp.where(self.sub == place, tile, value)
        return value

    def rows_beyond(self, hi, lo, j, y, second_kick):
        base = 4 * (j % 2)
        if second_kick:
            return pltpu.roll(hi, (-base - 3) % 8, 0) if y == 0 else jnp.zeros(hi.shape, F32)
        above, below = (-base - 2 * y) % 8, 7 - 2 * j - y
        above = pltpu.roll(hi, above, 0) if above else hi
        below = pltpu.roll(lo, below % 8, 0) if below % 8 else lo
        return jnp.where(self.sub < 2 - y, above, jnp.where(self.sub == 7, below, 0.0))

    def section(self, t, planes):
        S, ST, K = self.S, self.ST, self.K
        sweep, colour = divmod(t, 8)
        yp, xp = (colour // 2) % 2, colour % 2
        acc = jnp.zeros((8, self.lanes), F32)
        for z in planes:
            zi = z + 3
            stiff = ST[yp, xp, zi]
            local = []
            for c in (0, 1):
                along = S[c, yp, 1 - xp, zi]
                if xp == 0:
                    total = jnp.take_along_axis(along, self.before, axis=1) + pltpu.roll(along, self.lanes - 1, 1)
                else:
                    total = jnp.take_along_axis(along, self.after, axis=1) + pltpu.roll(along, 1, 1)
                across = S[c, 1 - yp, xp, zi]
                total = total + (across + pltpu.roll(across, 1 if yp == 0 else self.rows - 1, 0))
                total = total + (S[c, yp, xp, zi - 1] + S[c, yp, xp, zi + 1])
                local.append(stiff * total + K[2 * sweep + c, yp, xp, zi])
            square = local[0] * local[0] + local[1] * local[1]
            scale = lax.rsqrt(1.0 + square)
            for c in (0, 1):
                S[c, yp, xp, zi] = local[c] * scale
            if 0 <= z < self.depth:
                energy = (square * scale)[: self.half]
                acc = acc + sum(energy[8 * j : 8 * j + 8] for j in range(self.half // 8))
        return acc


def inner_planes(depth, t):
    phase = t // 4
    return range(2 + phase, depth - 1 - phase, 2)


def outer_planes(depth, t):
    phase = t // 4
    reach = 2 * (SWEEPS - 1 - t // 8)
    parity = phase % 2
    return [z for z in range(parity - reach, depth - parity + reach + 1, 2) if z not in inner_planes(depth, t)]


def build_kernel(*refs):
    own, other = refs[:3], refs[3:6]
    S, ST, K = refs[6:]
    depth, height, _ = own[2].shape
    rows = Rows(S, ST, K, depth, height)

    def two(p, carry):
        for field in ALL:
            for z in (2 * p, 2 * p + 1):
                for y in (0, 1):
                    a, b = (load_field(*side, field, z, pl.ds(y, height // 2, stride=2)) for side in (own, other))
                    rows.put(field, z + 3, y, 0, a, b)
        return carry

    lax.fori_loop(0, depth // 2, two, 0)


def build(own, other):
    depth, height, lanes = own[2].shape
    rows = -(-(height // 2 + 4) // 8) * 8
    planes = depth + 7
    return pl.pallas_call(
        build_kernel,
        out_shape=[
            jax.ShapeDtypeStruct((2, 2, 2, planes, rows, lanes), F32),
            jax.ShapeDtypeStruct((2, 2, planes, rows, lanes), F32),
            jax.ShapeDtypeStruct((2 * SWEEPS, 2, 2, planes, rows, lanes), F32),
        ],
        in_specs=[VMEM] * 6,
        out_specs=[VMEM] * 3,
        compiler_params=pltpu.CompilerParams(vmem_limit_bytes=8 << 20),
        cost_estimate=pl.CostEstimate(flops=30_000_000, bytes_accessed=10_000_000, transcendentals=0),
        name="build",
    )(*own, *other)


def middle_kernel(*refs):
    sides = refs[3:5]
    height = 2 * refs[5][0]
    S, ST, K, E = refs[6:]
    depth = S.shape[3] - 7
    rows = Rows(S, ST, K, depth, height)
    high = 5 * depth // 4

    def four(q, carry):
        for field in ALL:
            source = field if field in FIRST else field - 5
            for j in range(4):
                for y in (0, 1):
                    a, b = (
                        rows.rows_beyond(
                            side[high + source * (depth // 2) + 2 * q + j // 2],
                            side[source * (depth // 4) + q],
                            j,
                            y,
                            field not in FIRST,
                        )
                        for side in sides
                    )
                    rows.put(field, 4 * q + j + 3, y, height // 2, a, b)
        return carry

    lax.fori_loop(0, depth // 4, four, 0)
    for t in range(8 * SWEEPS):
        E[t] = rows.section(t, inner_planes(depth, t))


def middle(state, own, other, height):
    lanes = own.shape[-1]

    def kernel(*refs):
        middle_kernel(*refs[:5], (height // 2,), *refs[5:])

    return pl.pallas_call(
        kernel,
        out_shape=[jax.ShapeDtypeStruct(v.shape, F32) for v in state] + [jax.ShapeDtypeStruct((8 * SWEEPS, 8, lanes), F32)],
        in_specs=[VMEM] * 5,
        out_specs=[VMEM] * 4,
        input_output_aliases={0: 0, 1: 1, 2: 2},
        compiler_params=pltpu.CompilerParams(vmem_limit_bytes=8 << 20),
        cost_estimate=pl.CostEstimate(flops=30_000_000, bytes_accessed=10_000_000, transcendentals=0),
        name="middle",
    )(*state, own, other)


def last_kernel(*refs):
    E = refs[3]
    own, other = refs[4:7], refs[7:10]
    S, ST, K, out, energies, lines, final, sems = refs[10:]
    depth, height, lanes = out.shape[1:]
    rows = Rows(S, ST, K, depth, height)
    sides = (own, other)
    for c in range(2):
        for y in range(2):
            for x in range(2):
                S[c, y, x, 0] = jnp.zeros((rows.rows, lanes), F32)
                S[c, y, x, depth + 6] = jnp.zeros((rows.rows, lanes), F32)
    for which, listed, base, names in ((0, up_planes(depth), -depth, ("cuu", "cud")), (1, down_planes(), depth, ("cdu", "cdd"))):
        for n, (field, z) in enumerate(listed):
            for y in (0, 1):
                a, b = (
                    jnp.concatenate(
                        [
                            side[which][n, pl.ds(y, height // 2, stride=2), :],
                            rows.corner(side[2], names, n, y),
                        ],
                        axis=0,
                    )
                    for side in sides
                )
                rows.put(field, z + base + 3, y, 0, a, b)
    half = height // 2
    sent = []

    def send(start, stop):
        for z in range(start, stop):
            for c in (0, 1):
                for y in (0, 1):
                    value = jnp.where(rows.even[:half], S[c, y, 0, z + 3, :half], S[c, y, 1, z + 3, :half])
                    final[c, z, pl.ds(y, half, stride=2), :] = value
        part = pl.ds(start, stop - start)
        copy = pltpu.make_async_copy(final.at[:, part], out.at[:, part], sems.at[len(sent)])
        copy.start()
        sent.append(copy)

    low, high = 2 * SWEEPS, depth - 2 * SWEEPS + 1
    send(low, high)
    for t in range(8 * SWEEPS):
        acc = E[t] + rows.section(t, outer_planes(depth, t))
        mine = rows.lane % 2 == t % 2
        lines[pl.ds(t, 1), :] = jnp.sum(jnp.where(mine, acc, 0.0), axis=0, keepdims=True)

    send(0, low)
    send(high, depth)
    total = jnp.sum(lines[...], axis=1, keepdims=True)
    diagonal = lax.broadcasted_iota(jnp.int32, lines.shape, 0) == lax.broadcasted_iota(jnp.int32, lines.shape, 1)
    line = jnp.sum(jnp.where(diagonal, total, 0.0), axis=0, keepdims=True)
    energies[...] = jnp.broadcast_to(line, energies.shape)
    for copy in sent:
        copy.wait()


def last(state, own, other, shape, devices):
    lanes = shape[-1]
    results = pl.pallas_call(
        last_kernel,
        out_shape=[jax.ShapeDtypeStruct(v.shape, F32) for v in state[:3]]
        + [jax.ShapeDtypeStruct(shape, F32), jax.ShapeDtypeStruct((devices, lanes), F32)],
        in_specs=[VMEM] * 10,
        out_specs=[VMEM] * 3 + [pl.BlockSpec(memory_space=pltpu.HBM), VMEM],
        input_output_aliases={0: 0, 1: 1, 2: 2},
        scratch_shapes=[
            pltpu.VMEM((8 * SWEEPS, lanes), F32),
            pltpu.VMEM(shape, F32),
            pltpu.SemaphoreType.DMA((3,)),
        ],
        compiler_params=pltpu.CompilerParams(vmem_limit_bytes=8 << 20),
        cost_estimate=pl.CostEstimate(flops=30_000_000, bytes_accessed=10_000_000, transcendentals=0),
        name="last",
    )(*state, *own, *other)
    return results[3:]


def step(spins, kicks, stiffness):
    nz, ny, nx = (lax.axis_size(a) for a in ("gz", "gy", "gx"))
    devices = nz * ny * nx
    sites = jnp.float32(stiffness.size * devices // 8)

    def shift(value, even_core, odd_core):
        pairs = []
        for z in range(nz):
            for y in range(ny):
                for x in range(nx):
                    dz, dy = odd_core if x % 2 else even_core
                    pairs.append(((z * ny + y) * nx + x, ((z + dz) % nz * ny + (y + dy) % ny) * nx + x))
        return lax.ppermute(value, ("gz", "gy", "gx"), pairs)

    def swap(value):
        return lax.ppermute(value, "gx", [(i, i ^ 1) for i in range(nx)])

    lanes = stiffness.shape[-1]

    def beside(value):
        right = lax.ppermute(value, "gx", [((i + 1) % nx, i) for i in range(nx)])
        if nx == 2:
            return right
        left = lax.ppermute(value, "gx", [(i, (i + 1) % nx) for i in range(nx)])
        lane = lax.broadcasted_iota(jnp.int32, value.shape, value.ndim - 1)
        return jnp.where(lane < lanes // 2, right, left)

    raw = (spins, kicks, stiffness)
    zup, zdn = pack_faces(*raw)
    yup, ydn, mine = pack_edges(*raw, zup, zdn)
    first, second = share_out(lanes, mine, swap(mine))
    up, down, left, right = (1, 0), (-1, 0), (0, -1), (0, 1)
    zlo, zhi = shift(zup, up, up), shift(zdn, down, down)
    edges = join(shift(yup, right, right), shift(ydn, left, left))
    corners = stack_corners(lanes, shift(first, (-1, -1), (-1, 1)), shift(second, (1, -1), (1, 1)))
    beyond = beside(edges)
    other = tuple(beside(v) for v in raw)
    state = build(raw, other)
    state = middle(state, edges, beyond, stiffness.shape[1])
    corners, beyond = sort_corners(lanes, corners, swap(corners))
    if nx > 2:
        beyond = beside(corners)
    other = (beside(zlo), beside(zhi), beyond)
    final, energies = last(state, (zlo, zhi, corners), other, spins.shape, devices)
    parts = lax.all_to_all(energies, ("gz", "gy", "gx"), 0, 0, tiled=True)
    total = jnp.sum(parts, axis=0)[: 8 * SWEEPS]
    return (final, -total / sites)


def solution(mesh):
    placed = (P(None, "gz", "gy", "gx"), P(None, None, "gz", "gy", "gx"), P("gz", "gy", "gx"))
    return jax.shard_map(
        step,
        mesh=mesh,
        in_specs=placed,
        out_specs=(P(None, "gz", "gy", "gx"), P()),
        check_vma=False,
    )
```

```python
import functools

import jax
import jax.numpy as jnp
from jax import lax
from jax.experimental import pallas as pl
from jax.experimental.pallas import tpu as pltpu
from jax.sharding import PartitionSpec as P


SWEEPS = 2
FACE_GRANT = 56_000_000
EDGE_GRANT = 8_000_000
VMEM = pl.BlockSpec(memory_space=pltpu.VMEM)
F32 = jnp.float32

FIRST = (0, 1, 2, 3, 4)
ALL = (0, 1, 2, 3, 4, 5, 6)


def up_planes(depth):
    return [(f, z) for f in FIRST for z in (depth - 2, depth - 1)]


def down_planes():
    return [(f, z) for f in FIRST for z in (0, 1, 2)] + [(5, 0), (6, 0)]


CORNERS = {"cuu": (0, 1), "cud": (1, 2), "cdu": (3, 3), "cdd": (6, 5)}
CORNER_TILES = 11


def corner_rows(name):
    if name == "cuu":
        spins, first, second = {1: (-1, -2), 0: (-1,)}, {}, ()
    elif name == "cud":
        spins, first, second = {1: (0, 1, 2), 0: (0, 1)}, {1: (0,), 0: (0,)}, ()
    elif name == "cdu":
        spins, first, second = {0: (-1, -2, -3), 1: (-1, -2), 2: (-1,)}, {0: (-1, -2)}, ()
    else:
        spins, first, second = {0: (0, 1, 2, 3), 1: (0, 1, 2), 2: (0, 1)}, {0: (0, 1, 2), 1: (0,), 2: (0,)}, (0,)
    planes = 2 if name[1] == "u" else 3
    listed = [(planes * f + z, r) for f in FIRST for z, rows in (spins if f < 2 else first).items() for r in rows]
    return listed + [(n, r) for n in (15, 16) for r in second]


def place_of(planes, n, height):
    short = [m for m, (f, z) in enumerate(planes) if f < 2 and z % 2 == 0]
    whole = [m for m in range(len(planes)) if m not in short]
    half = height // 2
    packed = half + packed_even(half)
    if n in short:
        return len(whole) * height + short.index(n) * packed, True
    return whole.index(n) * height, False


def packed_even(half):
    return -(-half // 16) * 8


def face_rows(planes, height):
    short = sum(f < 2 and z % 2 == 0 for f, z in planes)
    return (len(planes) - short) * height + short * (height // 2 + packed_even(height // 2))


def load_field(s_ref, k_ref, st_ref, field, z, rows=slice(None)):
    return field_ref(s_ref, k_ref, st_ref, field)[z, rows, :]


def field_ref(s_ref, k_ref, st_ref, field):
    if field < 2:
        return s_ref.at[field]
    if field == 2:
        return st_ref
    return k_ref.at[(field - 3) // 2, (field - 3) % 2]


def copy_all(moves, sems):
    copies = [pltpu.make_async_copy(a, b, sems.at[i]) for i, (a, b) in enumerate(moves)]
    for c in copies:
        c.start()
    for c in copies:
        c.wait()


def face_kernel(s_ref, k_ref, st_ref, zup, zdn, far, raw, sems):
    depth, height, lanes = st_ref.shape
    half = height // 2
    keep = packed_even(half)
    get = functools.partial(field_ref, s_ref, k_ref, st_ref)
    moves = [(s_ref.at[:, depth - 3], far.at[0]), (s_ref.at[:, 3], far.at[1])]
    packed = []
    for out, planes in ((zup, up_planes(depth)), (zdn, down_planes())):
        for n, (f, z) in enumerate(planes):
            start, short = place_of(planes, n, height)
            if short:
                moves.append((get(f).at[z], raw.at[len(packed)]))
                packed.append((out, start))
            else:
                moves.append((get(f).at[z], out.at[pl.ds(start, height)]))
    copy_all(moves, sems)
    even = lax.broadcasted_iota(jnp.int32, (half - keep, lanes), 1) % 2 == 0
    for m, (out, start) in enumerate(packed):
        rows = raw[m, pl.ds(0, half, stride=2), :]
        rest = pltpu.roll(rows[keep:], lanes - 1, 1)
        out[start : start + half] = raw[m, pl.ds(1, half, stride=2), :]
        out[start + half : start + half + half - keep] = jnp.where(even, rest, rows[: half - keep])
        out[start + 2 * half - keep : start + half + keep] = rows[half - keep : keep]
    for out, planes, z, side in ((zup, up_planes(depth), depth - 2, 0), (zdn, down_planes(), 2, 1)):
        stiff, _ = place_of(planes, planes.index((2, z)), height)
        for c in (0, 1):
            start, _ = place_of(planes, planes.index((3 + c, z)), height)
            out[start : start + height] = out[start : start + height] + out[stiff : stiff + height] * far[side, c]


def edge_kernel(s_ref, k_ref, st_ref, zup, zdn, up, down, corners, s_low, s_high, k_low, k_high, t_low, t_high, sems):
    depth, height, lanes = st_ref.shape
    first, last = pl.ds(0, 8), pl.ds(height - 8, 8)
    copy_all(
        [
            (s_ref.at[:, :, first], s_low),
            (s_ref.at[:, :, last], s_high),
            (k_ref.at[:, :, :, first], k_low),
            (k_ref.at[0, :, :, last], k_high),
            (st_ref.at[:, first], t_low),
            (st_ref.at[:, last], t_high),
        ],
        sems,
    )
    sub = lax.broadcasted_iota(jnp.int32, (8, lanes), 0)
    quad = sub % 4
    order = (quad % 2) * 2 + quad // 2
    lower = sub < 4

    def merge(a, b, base):
        a = jnp.take_along_axis(a, order + base, axis=0)
        b = jnp.take_along_axis(b, order + base, axis=0)
        return jnp.where(lower, a, b)

    for name, (start, count) in CORNERS.items():
        src, planes = (zup, up_planes(depth)) if name[1] == "u" else (zdn, down_planes())
        tiles = [jnp.zeros((8, lanes), F32)] * count
        for i, (n, r) in enumerate(corner_rows(name)):
            place = r if r >= 0 else 8 + r
            field, z = planes[n]
            if field < 2:
                value = s_low[field, z] if r >= 0 else s_high[field, z]
            else:
                base, _ = place_of(planes, n, height)
                base = base if r >= 0 else base + height - 8
                value = src[base : base + 8]
            shift = (i - place) % 8
            value = pltpu.roll(value, shift, 0) if shift else value
            tiles[i // 8] = jnp.where(sub == i % 8, value, tiles[i // 8])
        for i in range(count):
            corners[start + i] = tiles[i]

    def row(field, z, is_low):
        s, k, t = (s_low, k_low, t_low) if is_low else (s_high, k_high, t_high)
        if field < 2:
            return s[field, z]
        if field == 2:
            return t[z]
        c = (field - 3) % 2
        if not is_low:
            return k[c, z] + jnp.where(sub == 6, t[z] * pltpu.roll(s[c, z], 1, 0), 0.0)
        if field > 4:
            return k[1, c, z]
        return k[0, c, z] + jnp.where(sub == 2, t[z] * pltpu.roll(s[c, z], 7, 0), 0.0)

    for field in FIRST:
        for p in range(depth // 2):
            tile = merge(row(field, 2 * p, True), row(field, 2 * p + 1, True), 0)
            if field < 2:
                a, b = (pltpu.roll(row(5 + field, 2 * p + i, True), 3 + 4 * i, 0) for i in (0, 1))
                tile = jnp.where(quad == 3, jnp.where(lower, a, b), tile)
            down[field * (depth // 2) + p] = tile
        for q in range(depth // 4):
            tile = row(field, 4 * q + 3, False)
            for i in range(3):
                tile = jnp.where(sub // 2 == i, pltpu.roll(row(field, 4 * q + i, False), (2 * i + 2) % 8, 0), tile)
            up[field * (depth // 4) + q] = tile


def pack_faces(spins, kicks, stiffness):
    depth, height, lanes = stiffness.shape
    lists = (up_planes(depth), down_planes())
    return pl.pallas_call(
        face_kernel,
        out_shape=[jax.ShapeDtypeStruct((face_rows(p, height), lanes), F32) for p in lists],
        in_specs=[pl.BlockSpec(memory_space=pltpu.HBM)] * 3,
        out_specs=[VMEM] * 2,
        scratch_shapes=[
            pltpu.VMEM((2, 2, height, lanes), F32),
            pltpu.VMEM((6, height, lanes), F32),
            pltpu.SemaphoreType.DMA((29,)),
        ],
        compiler_params=pltpu.CompilerParams(vmem_limit_bytes=FACE_GRANT),
        cost_estimate=pl.CostEstimate(flops=1_000_000, bytes_accessed=1_000_000, transcendentals=0),
        name="faces",
    )(spins, kicks, stiffness)


def pack_edges(spins, kicks, stiffness, zup, zdn):
    depth, _, lanes = stiffness.shape
    return pl.pallas_call(
        edge_kernel,
        out_shape=[jax.ShapeDtypeStruct((n, 8, lanes), F32) for n in (5 * depth // 4, 5 * depth // 2, CORNER_TILES)],
        in_specs=[pl.BlockSpec(memory_space=pltpu.HBM)] * 3 + [VMEM] * 2,
        out_specs=[VMEM] * 3,
        scratch_shapes=[
            pltpu.VMEM((2, depth, 8, lanes), F32),
            pltpu.VMEM((2, depth, 8, lanes), F32),
            pltpu.VMEM((SWEEPS, 2, depth, 8, lanes), F32),
            pltpu.VMEM((2, depth, 8, lanes), F32),
            pltpu.VMEM((depth, 8, lanes), F32),
            pltpu.VMEM((depth, 8, lanes), F32),
            pltpu.SemaphoreType.DMA((6,)),
        ],
        compiler_params=pltpu.CompilerParams(vmem_limit_bytes=EDGE_GRANT),
        cost_estimate=pl.CostEstimate(flops=1_000_000, bytes_accessed=2_000_000, transcendentals=0),
        name="edges",
    )(spins, kicks, stiffness, zup, zdn)


def small_call(kernel, shapes, *args):
    return pl.pallas_call(
        kernel,
        out_shape=[jax.ShapeDtypeStruct(s, F32) for s in shapes],
        in_specs=[VMEM] * len(args),
        out_specs=[VMEM] * len(shapes),
        compiler_params=pltpu.CompilerParams(vmem_limit_bytes=4 << 20),
        cost_estimate=pl.CostEstimate(flops=100_000, bytes_accessed=1_000_000, transcendentals=0),
    )(*args)


def per_core(moves):
    core = lax.axis_index("gx") % 2
    for c in (0, 1):

        @pl.when(core == c)
        def _():
            for target, at, source, start, count in moves[c]:
                target[at : at + count] = source[start : start + count]


def share_out(lanes, mine, pair):
    def spread(mine, pair, first, second):
        moves = ([], [])
        for core, parts in ((0, (("cdd", first), ("cud", second))), (1, (("cdu", first), ("cuu", second)))):
            for name, target in parts:
                start, count = CORNERS[name]
                moves[core].append((target, 0, mine, start, count))
                moves[core].append((target, target.shape[0] // 2, pair, start, count))
        per_core(moves)

    return small_call(spread, [(10, 8, lanes), (4, 8, lanes)], mine, pair)


def join(lo, hi):
    def join_edges(lo, hi, out):
        out[: lo.shape[0]] = lo[...]
        out[lo.shape[0] :] = hi[...]

    return small_call(join_edges, [(lo.shape[0] + hi.shape[0], *lo.shape[1:])], lo, hi)[0]


def stack_corners(lanes, first, second):
    def stack(first, second, out):
        out[:10] = first[...]
        out[10:] = second[...]

    return small_call(stack, [(14, 8, lanes)], first, second)[0]


def sort_corners(lanes, got, pair):
    def sort_c(got, pair, own, other):
        moves = ([], [])
        for name, start, half, core in (("cdd", 0, 5, 0), ("cdu", 0, 5, 1), ("cud", 10, 2, 0), ("cuu", 10, 2, 1)):
            place, count = CORNERS[name]
            for c in (0, 1):
                source, flip = (got, 0) if c == core else (pair, half)
                moves[c].append((own, place, source, start + flip, count))
                moves[c].append((other, place, source, start + half - flip, count))
        per_core(moves)

    return small_call(sort_c, [(CORNER_TILES, 8, lanes)] * 2, got, pair)


class Rows:
    def __init__(self, S, ST, K, depth, height):
        self.S, self.ST, self.K = S, ST, K
        self.depth, self.height = depth, height
        self.half = height // 2
        self.rows, self.lanes = S.shape[4:]
        lane = lax.broadcasted_iota(jnp.int32, (8, self.lanes), 1)
        self.lane = lane
        self.sub = lax.broadcasted_iota(jnp.int32, (8, self.lanes), 0)
        self.even = lax.broadcasted_iota(jnp.int32, (self.rows, self.lanes), 1) % 2 == 0
        end = self.lanes - 1
        before = jnp.where(lane == 0, 0, jnp.where(lane == 1, end, lane - 1))
        after = jnp.where(lane == 0, 0, jnp.where(lane == end, 1, lane + 1))
        self.before = jnp.concatenate([before] * (self.rows // 8), axis=0)
        self.after = jnp.concatenate([after] * (self.rows // 8), axis=0)

    def put(self, field, zi, y, start, a, b):
        b = pltpu.roll(b, 1, 1)
        even = self.even[: a.shape[0]]
        for x in (0, 1):
            value = jnp.where(even, a, b) if x == 0 else jnp.where(even, b, a)
            at = (y, x, zi, pl.ds(start, a.shape[0]))
            if field < 2:
                self.S[(field, *at)] = value
            elif field == 2:
                self.ST[at] = value
            else:
                self.K[(field - 3, *at)] = value

    def face(self, ref, planes, n, y):
        start, packed = place_of(planes, n, self.height)
        if not packed:
            return ref[pl.ds(start + y, self.half, stride=2), :]
        if y == 1:
            return ref[start : start + self.half]
        keep = packed_even(self.half)
        value = ref[start + self.half : start + self.half + keep]
        return jnp.concatenate([value, pltpu.roll(value[: self.half - keep], 1, 1)], axis=0)

    def corner(self, tiles, names, n, y):
        value = jnp.zeros((8, self.lanes), F32)
        for name in names:
            for i, (m, r) in enumerate(corner_rows(name)):
                if m == n and r % 2 == y:
                    place = r // 2 if r >= 0 else {-1: 7, -2: 7, -3: 6}[r]
                    tile = tiles[CORNERS[name][0] + i // 8]
                    shift = (place - i) % 8
                    tile = pltpu.roll(tile, shift, 0) if shift else tile
                    value = jnp.where(self.sub == place, tile, value)
        return value

    def rows_beyond(self, hi, lo, j, y, second_kick):
        base = 4 * (j % 2)
        if second_kick:
            return pltpu.roll(hi, (-base - 3) % 8, 0) if y == 0 else jnp.zeros(hi.shape, F32)
        above, below = (-base - 2 * y) % 8, 7 - 2 * j - y
        above = pltpu.roll(hi, above, 0) if above else hi
        below = pltpu.roll(lo, below % 8, 0) if below % 8 else lo
        return jnp.where(self.sub < 2 - y, above, jnp.where(self.sub == 7, below, 0.0))

    def section(self, t, planes):
        S, ST, K = self.S, self.ST, self.K
        sweep, colour = divmod(t, 8)
        yp, xp = (colour // 2) % 2, colour % 2
        acc = jnp.zeros((8, self.lanes), F32)
        for z in planes:
            zi = z + 3
            stiff = ST[yp, xp, zi]
            local = []
            for c in (0, 1):
                along = S[c, yp, 1 - xp, zi]
                if xp == 0:
                    total = jnp.take_along_axis(along, self.before, axis=1) + pltpu.roll(along, self.lanes - 1, 1)
                else:
                    total = jnp.take_along_axis(along, self.after, axis=1) + pltpu.roll(along, 1, 1)
                across = S[c, 1 - yp, xp, zi]
                total = total + (across + pltpu.roll(across, 1 if yp == 0 else self.rows - 1, 0))
                total = total + (S[c, yp, xp, zi - 1] + S[c, yp, xp, zi + 1])
                local.append(stiff * total + K[2 * sweep + c, yp, xp, zi])
            square = local[0] * local[0] + local[1] * local[1]
            scale = lax.rsqrt(1.0 + square)
            for c in (0, 1):
                S[c, yp, xp, zi] = local[c] * scale
            if 0 <= z < self.depth:
                energy = (square * scale)[: self.half]
                acc = acc + sum(energy[8 * j : 8 * j + 8] for j in range(self.half // 8))
        return acc


def inner_planes(depth, t):
    phase = t // 4
    return range(2 + phase, depth - 1 - phase, 2)


def outer_planes(depth, t):
    phase = t // 4
    reach = 2 * (SWEEPS - 1 - t // 8)
    parity = phase % 2
    return [z for z in range(parity - reach, depth - parity + reach + 1, 2) if z not in inner_planes(depth, t)]


def build_kernel(*refs):
    own, other = refs[:3], refs[3:6]
    S, ST, K = refs[6:]
    depth, height, _ = own[2].shape
    rows = Rows(S, ST, K, depth, height)

    def two(p, carry):
        for field in ALL:
            for z in (2 * p, 2 * p + 1):
                for y in (0, 1):
                    a, b = (load_field(*side, field, z, pl.ds(y, height // 2, stride=2)) for side in (own, other))
                    rows.put(field, z + 3, y, 0, a, b)
        return carry

    lax.fori_loop(0, depth // 2, two, 0)


def build(own, other):
    depth, height, lanes = own[2].shape
    rows = -(-(height // 2 + 4) // 8) * 8
    planes = depth + 7
    return pl.pallas_call(
        build_kernel,
        out_shape=[
            jax.ShapeDtypeStruct((2, 2, 2, planes, rows, lanes), F32),
            jax.ShapeDtypeStruct((2, 2, planes, rows, lanes), F32),
            jax.ShapeDtypeStruct((2 * SWEEPS, 2, 2, planes, rows, lanes), F32),
        ],
        in_specs=[VMEM] * 6,
        out_specs=[VMEM] * 3,
        compiler_params=pltpu.CompilerParams(vmem_limit_bytes=8 << 20),
        cost_estimate=pl.CostEstimate(flops=30_000_000, bytes_accessed=10_000_000, transcendentals=0),
        name="build",
    )(*own, *other)


def middle_kernel(*refs):
    sides = refs[3:5]
    height = 2 * refs[5][0]
    S, ST, K, E = refs[6:]
    depth = S.shape[3] - 7
    rows = Rows(S, ST, K, depth, height)
    high = 5 * depth // 4

    def four(q, carry):
        for field in ALL:
            source = field if field in FIRST else field - 5
            for j in range(4):
                for y in (0, 1):
                    a, b = (
                        rows.rows_beyond(
                            side[high + source * (depth // 2) + 2 * q + j // 2],
                            side[source * (depth // 4) + q],
                            j,
                            y,
                            field not in FIRST,
                        )
                        for side in sides
                    )
                    rows.put(field, 4 * q + j + 3, y, height // 2, a, b)
        return carry

    lax.fori_loop(0, depth // 4, four, 0)
    for t in range(8 * SWEEPS):
        E[t] = rows.section(t, inner_planes(depth, t))


def middle(state, own, other, height):
    lanes = own.shape[-1]

    def kernel(*refs):
        middle_kernel(*refs[:5], (height // 2,), *refs[5:])

    return pl.pallas_call(
        kernel,
        out_shape=[jax.ShapeDtypeStruct(v.shape, F32) for v in state] + [jax.ShapeDtypeStruct((8 * SWEEPS, 8, lanes), F32)],
        in_specs=[VMEM] * 5,
        out_specs=[VMEM] * 4,
        input_output_aliases={0: 0, 1: 1, 2: 2},
        compiler_params=pltpu.CompilerParams(vmem_limit_bytes=8 << 20),
        cost_estimate=pl.CostEstimate(flops=30_000_000, bytes_accessed=10_000_000, transcendentals=0),
        name="middle",
    )(*state, own, other)


def last_kernel(*refs):
    E = refs[3]
    own, other = refs[4:7], refs[7:10]
    S, ST, K, out, energies, lines, final, sems = refs[10:]
    depth, height, lanes = out.shape[1:]
    rows = Rows(S, ST, K, depth, height)
    sides = (own, other)
    for c in range(2):
        for y in range(2):
            for x in range(2):
                S[c, y, x, 0] = jnp.zeros((rows.rows, lanes), F32)
                S[c, y, x, depth + 6] = jnp.zeros((rows.rows, lanes), F32)
    for which, listed, base, names in ((0, up_planes(depth), -depth, ("cuu", "cud")), (1, down_planes(), depth, ("cdu", "cdd"))):
        for n, (field, z) in enumerate(listed):
            for y in (0, 1):
                a, b = (
                    jnp.concatenate(
                        [
                            rows.face(side[which], listed, n, y),
                            rows.corner(side[2], names, n, y),
                        ],
                        axis=0,
                    )
                    for side in sides
                )
                rows.put(field, z + base + 3, y, 0, a, b)
    half = height // 2
    sent = []

    def send(start, stop):
        for z in range(start, stop):
            for c in (0, 1):
                for y in (0, 1):
                    value = jnp.where(rows.even[:half], S[c, y, 0, z + 3, :half], S[c, y, 1, z + 3, :half])
                    final[c, z, pl.ds(y, half, stride=2), :] = value
        part = pl.ds(start, stop - start)
        copy = pltpu.make_async_copy(final.at[:, part], out.at[:, part], sems.at[len(sent)])
        copy.start()
        sent.append(copy)

    low, high = 2 * SWEEPS, depth - 2 * SWEEPS + 1
    send(low, high)
    for t in range(8 * SWEEPS):
        acc = E[t] + rows.section(t, outer_planes(depth, t))
        mine = rows.lane % 2 == t % 2
        lines[pl.ds(t, 1), :] = jnp.sum(jnp.where(mine, acc, 0.0), axis=0, keepdims=True)

    send(0, low)
    send(high, depth)
    total = jnp.sum(lines[...], axis=1, keepdims=True)
    diagonal = lax.broadcasted_iota(jnp.int32, lines.shape, 0) == lax.broadcasted_iota(jnp.int32, lines.shape, 1)
    line = jnp.sum(jnp.where(diagonal, total, 0.0), axis=0, keepdims=True)
    energies[...] = jnp.broadcast_to(line, energies.shape)
    for copy in sent:
        copy.wait()


def last(state, own, other, shape, devices):
    lanes = shape[-1]
    results = pl.pallas_call(
        last_kernel,
        out_shape=[jax.ShapeDtypeStruct(v.shape, F32) for v in state[:3]]
        + [jax.ShapeDtypeStruct(shape, F32), jax.ShapeDtypeStruct((devices, lanes), F32)],
        in_specs=[VMEM] * 10,
        out_specs=[VMEM] * 3 + [pl.BlockSpec(memory_space=pltpu.HBM), VMEM],
        input_output_aliases={0: 0, 1: 1, 2: 2},
        scratch_shapes=[
            pltpu.VMEM((8 * SWEEPS, lanes), F32),
            pltpu.VMEM(shape, F32),
            pltpu.SemaphoreType.DMA((3,)),
        ],
        compiler_params=pltpu.CompilerParams(vmem_limit_bytes=8 << 20),
        cost_estimate=pl.CostEstimate(flops=30_000_000, bytes_accessed=10_000_000, transcendentals=0),
        name="last",
    )(*state, *own, *other)
    return results[3:]


def step(spins, kicks, stiffness):
    nz, ny, nx = (lax.axis_size(a) for a in ("gz", "gy", "gx"))
    devices = nz * ny * nx
    sites = jnp.float32(stiffness.size * devices // 8)

    def shift(value, even_core, odd_core):
        pairs = []
        for z in range(nz):
            for y in range(ny):
                for x in range(nx):
                    dz, dy = odd_core if x % 2 else even_core
                    pairs.append(((z * ny + y) * nx + x, ((z + dz) % nz * ny + (y + dy) % ny) * nx + x))
        return lax.ppermute(value, ("gz", "gy", "gx"), pairs)

    def swap(value):
        return lax.ppermute(value, "gx", [(i, i ^ 1) for i in range(nx)])

    lanes = stiffness.shape[-1]

    def beside(value):
        right = lax.ppermute(value, "gx", [((i + 1) % nx, i) for i in range(nx)])
        if nx == 2:
            return right
        left = lax.ppermute(value, "gx", [(i, (i + 1) % nx) for i in range(nx)])
        lane = lax.broadcasted_iota(jnp.int32, value.shape, value.ndim - 1)
        return jnp.where(lane < lanes // 2, right, left)

    raw = (spins, kicks, stiffness)
    zup, zdn = pack_faces(*raw)
    yup, ydn, mine = pack_edges(*raw, zup, zdn)
    first, second = share_out(lanes, mine, swap(mine))
    up, down, left, right = (1, 0), (-1, 0), (0, -1), (0, 1)
    zlo, zhi = shift(zup, up, up), shift(zdn, down, down)
    edges = join(shift(yup, right, right), shift(ydn, left, left))
    corners = stack_corners(lanes, shift(first, (-1, -1), (-1, 1)), shift(second, (1, -1), (1, 1)))
    beyond = beside(edges)
    other = tuple(beside(v) for v in raw)
    state = build(raw, other)
    state = middle(state, edges, beyond, stiffness.shape[1])
    corners, beyond = sort_corners(lanes, corners, swap(corners))
    if nx > 2:
        beyond = beside(corners)
    other = (beside(zlo), beside(zhi), beyond)
    final, energies = last(state, (zlo, zhi, corners), other, spins.shape, devices)
    parts = lax.all_to_all(energies, ("gz", "gy", "gx"), 0, 0, tiled=True)
    total = jnp.sum(parts, axis=0)[: 8 * SWEEPS]
    return (final, -total / sites)


def solution(mesh):
    placed = (P(None, "gz", "gy", "gx"), P(None, None, "gz", "gy", "gx"), P("gz", "gy", "gx"))
    return jax.shard_map(
        step,
        mesh=mesh,
        in_specs=placed,
        out_specs=(P(None, "gz", "gy", "gx"), P()),
        check_vma=False,
    )
```
